32 devices in a mesh: dp: 1 (over z), tp: 32 (over y, x, core).
Axes of the slice: x: 4, y: 4, z: 1, core: 2. Of those that a mesh axis runs over, the one named last changes fastest.
The devices are a block of a 4x4x8 slice.
Arguments:
- x_in: bfloat16 [512, 4096], P('dp')
- lengths: int32 [512], P('dp')
- norm_gain: bfloat16 [2, 4096], replicated
- w_q: bfloat16 [2, 4096, 4096], P(None, None, 'tp')
- w_k: bfloat16 [2, 4096, 4096], P(None, None, 'tp')
- w_v: bfloat16 [2, 4096, 4096], P(None, None, 'tp')
- w_o: bfloat16 [2, 4096, 4096], P(None, 'tp')
- w_gate: bfloat16 [2, 4096, 11008], P(None, None, 'tp')
- w_up: bfloat16 [2, 4096, 11008], P(None, None, 'tp')
- w_down: bfloat16 [2, 11008, 4096], P(None, 'tp')
- k_cache: bfloat16 [2, 512, 32, 32, 128], P(None, 'dp', None, 'tp')
- v_cache: bfloat16 [2, 512, 32, 32, 128], P(None, 'dp', None, 'tp')
Outputs:
- output: bfloat16 [512, 4096], P('dp')
All inputs are finite; a program needn't handle non-finite values.
Results may differ from the reference program's by a relative error of at most 0.0175018.
Values are sent between devices in bfloat16 or wider.
A program may use at most 768 MiB of HBM per device.

```python
import math
import jax
import jax.numpy as jnp
from jax import lax

D = 4096
HEADS = 32
KV_HEADS = 32
FF = 11008
HEAD = 128
BATCH = 512
SEQ = 32
LAYERS = 2
ROPE_BASE = 500000
NORM_EPS = 1e-5
GROUP = HEADS // KV_HEADS
LOG_LEVELS = int(math.log2(SEQ)) + 1


def draw_lengths(len_key):
    exp_key, val_key, top_key = jax.random.split(len_key, 3)
    span_exp = jax.random.randint(exp_key, (BATCH,), 0, LOG_LEVELS)
    span_limit = jnp.minimum(jnp.left_shift(jnp.ones_like(span_exp), span_exp), SEQ - 1)
    drawn_len = 1 + jax.random.randint(val_key, (BATCH,), 0, span_limit)
    full_slot = jax.random.randint(top_key, (), 0, BATCH)
    return jnp.where(jnp.arange(BATCH) == full_slot, SEQ - 1, drawn_len).astype(jnp.int32)


def setup_inputs(seed: int = 0, part: int = 0) -> dict:
    base_key = jax.random.key(seed)
    shared_keys = jax.random.split(base_key, 8)
    own_keys = jax.random.split(jax.random.fold_in(base_key, part), 4)
    q_width = HEADS * HEAD
    kv_width = KV_HEADS * HEAD

    def draw_weight(key_index, arr_shape, std_scale):
        return (jax.random.normal(shared_keys[key_index], arr_shape, jnp.float32) * std_scale).astype(jnp.bfloat16)

    return {
        'x_in': jax.random.normal(own_keys[0], (BATCH, D), jnp.float32).astype(jnp.bfloat16),
        'lengths': draw_lengths(own_keys[1]),
        'norm_gain': (1.0 + 0.3 * jax.random.normal(shared_keys[0], (LAYERS, D), jnp.float32)).astype(jnp.bfloat16),
        'w_q': draw_weight(1, (LAYERS, D, q_width), D ** -0.5),
        'w_k': draw_weight(2, (LAYERS, D, kv_width), 2.0 * D ** -0.5),
        'w_v': draw_weight(3, (LAYERS, D, kv_width), D ** -0.5),
        'w_o': draw_weight(4, (LAYERS, q_width, D), 2.0 * q_width ** -0.5),
        'w_gate': draw_weight(5, (LAYERS, D, FF), D ** -0.5),
        'w_up': draw_weight(6, (LAYERS, D, FF), D ** -0.5),
        'w_down': draw_weight(7, (LAYERS, FF, D), FF ** -0.5),
        'k_cache': (2.0 * jax.random.normal(own_keys[2], (LAYERS, BATCH, SEQ, KV_HEADS, HEAD), jnp.float32)).astype(jnp.bfloat16),
        'v_cache': jax.random.normal(own_keys[3], (LAYERS, BATCH, SEQ, KV_HEADS, HEAD), jnp.float32).astype(jnp.bfloat16),
    }


def rms_norm(x_res, gain_row):
    x_f32 = x_res.astype(jnp.float32)
    inv_rms = lax.rsqrt(jnp.mean(x_f32 * x_f32, axis=-1, keepdims=True) + NORM_EPS)
    return (x_f32 * inv_rms * gain_row.astype(jnp.float32)).astype(jnp.bfloat16)


def rope_rotate(head_vecs, positions):
    half_dim = HEAD // 2
    inv_freq = 1.0 / (ROPE_BASE ** (jnp.arange(0, HEAD, 2).astype(jnp.float32) / HEAD))
    angles = positions.astype(jnp.float32)[:, None] * inv_freq[None, :]
    cos_ang = jnp.cos(angles)[:, None, :]
    sin_ang = jnp.sin(angles)[:, None, :]
    vec_f32 = head_vecs.astype(jnp.float32)
    rot_first = vec_f32[..., :half_dim]
    rot_second = vec_f32[..., half_dim:]
    return jnp.concatenate([rot_first * cos_ang - rot_second * sin_ang, rot_second * cos_ang + rot_first * sin_ang], axis=-1).astype(jnp.bfloat16)


def decode_attention(q_rot, k_rot, v_new, k_layer, v_layer, lengths):
    attn_scale = HEAD ** -0.5
    q_f32 = q_rot.astype(jnp.float32)
    cache_logits = jnp.einsum('bkgd,bskd->bkgs', q_f32, k_layer.astype(jnp.float32)) * attn_scale
    valid_mask = jnp.arange(SEQ)[None, :] < lengths[:, None]
    cache_logits = jnp.where(valid_mask[:, None, None, :], cache_logits, -jnp.inf)
    self_logit = jnp.einsum('bkgd,bkd->bkg', q_f32, k_rot.astype(jnp.float32)) * attn_scale
    row_peak = jnp.maximum(jnp.max(cache_logits, axis=-1), self_logit)
    cache_w = jnp.exp(cache_logits - row_peak[..., None])
    self_w = jnp.exp(self_logit - row_peak)
    prob_denom = jnp.sum(cache_w, axis=-1) + self_w
    cache_p = (cache_w / prob_denom[..., None]).astype(jnp.bfloat16)
    self_p = (self_w / prob_denom).astype(jnp.bfloat16)
    cache_part = jnp.einsum('bkgs,bskd->bkgd', cache_p.astype(jnp.float32), v_layer.astype(jnp.float32))
    self_part = self_p.astype(jnp.float32)[..., None] * v_new.astype(jnp.float32)[:, :, None, :]
    return (cache_part + self_part).astype(jnp.bfloat16)


def reference(x_in, lengths, norm_gain, w_q, w_k, w_v, w_o, w_gate, w_up, w_down, k_cache, v_cache):
    def layer_step(x_res, layer_args):
        gain_row, wq_layer, wk_layer, wv_layer, wo_layer, wg_layer, wu_layer, wd_layer, k_layer, v_layer = layer_args
        normed = rms_norm(x_res, gain_row)
        q_proj = jnp.dot(normed, wq_layer, preferred_element_type=jnp.float32).astype(jnp.bfloat16).reshape(BATCH, HEADS, HEAD)
        k_proj = jnp.dot(normed, wk_layer, preferred_element_type=jnp.float32).astype(jnp.bfloat16).reshape(BATCH, KV_HEADS, HEAD)
        v_new = jnp.dot(normed, wv_layer, preferred_element_type=jnp.float32).astype(jnp.bfloat16).reshape(BATCH, KV_HEADS, HEAD)
        q_rot = rope_rotate(q_proj, lengths).reshape(BATCH, KV_HEADS, GROUP, HEAD)
        k_rot = rope_rotate(k_proj, lengths)
        attn_flat = decode_attention(q_rot, k_rot, v_new, k_layer, v_layer, lengths).reshape(BATCH, HEADS * HEAD)
        attn_proj = jnp.dot(attn_flat, wo_layer, preferred_element_type=jnp.float32)
        gate_act = jnp.dot(normed, wg_layer, preferred_element_type=jnp.float32).astype(jnp.bfloat16)
        up_act = jnp.dot(normed, wu_layer, preferred_element_type=jnp.float32).astype(jnp.bfloat16)
        mlp_hidden = (jax.nn.silu(gate_act.astype(jnp.float32)) * up_act.astype(jnp.float32)).astype(jnp.bfloat16)
        mlp_proj = jnp.dot(mlp_hidden, wd_layer, preferred_element_type=jnp.float32)
        x_next = (x_res.astype(jnp.float32) + attn_proj + mlp_proj).astype(jnp.bfloat16)
        return x_next, None

    scan_result = lax.scan(layer_step, x_in, (norm_gain, w_q, w_k, w_v, w_o, w_gate, w_up, w_down, k_cache, v_cache))
    return scan_result[0]
```

```python
import functools
import math

import jax
import jax.numpy as jnp
from jax import lax
from jax.experimental import pallas as pl
from jax.experimental.pallas import tpu as pltpu
from jax.sharding import PartitionSpec as P

NORM_EPS = 1e-5
ROPE_BASE = 500000.0
F32 = jnp.float32
BF16 = jnp.bfloat16
NT = (((1,), (1,)), ((), ()))
BLOCKS = 2
TILE = 256


def wait_bytes(ref, sem):
    pltpu.make_async_copy(ref, ref, sem).wait()


def layers_kernel(side, x_hbm, len_ref, cos_ref, sin_ref, gain_ref, wq, wk, wv, wo, wg, wu, wd, kc, vc, out_ref,
                  a_buf, wqkv, wgu, wod, kbuf, vbuf, q_s, k_s, v_s, self_s, h_buf, send, recv, x_own, st_send, st_recv,
                  x_sem, w_sem, wo_sem, wp_ssem, wp_rsem, c_sem, own_sem, h_ssem, h_rsem, rs_ssem, rs_rsem, st_sem, ag_ssem, ag_rsem, d_ssem, d_rsem):
    layers, width = wq.shape[0], wq.shape[1]
    head = wq.shape[2]
    ff = wd.shape[1]
    half = width // 2
    quarter = width // 4
    toks = x_hbm.shape[3]
    chips = side * side
    rows = chips * toks
    seq = kc.shape[1] // (BLOCKS * rows)
    ff_tiles = wgu.shape[1] // TILE
    kdim = h_buf.shape[3]
    scale = head ** -0.5

    me = lax.axis_index('tp')
    core = lax.rem(me, 2)
    chip = lax.div(me, 2)
    px = lax.rem(chip, side)
    py = lax.div(chip, side)
    other = 1 - core

    def dev(y, x, c):
        return {'tp': (y * side + x) * 2 + c}

    def shift(p, d):
        return lax.rem(p + d + side, side)

    partner = dev(py, px, other)
    my_cols = pl.ds(pl.multiple_of(core * half, half), half)
    other_cols = pl.ds(pl.multiple_of(other * half, half), half)

    def part_cols(hf, c):
        return pl.ds(pl.multiple_of(c * half + hf * quarter, quarter), quarter)

    def k_rows(c, start, n):
        return pl.ds(pl.multiple_of(c * kdim + start, 8), n)

    def x_load(b):
        return pltpu.make_async_copy(x_hbm.at[b], out_ref.at[b], x_sem.at[b])

    def qkv_loads(l):
        return [pltpu.make_async_copy(w.at[l], wqkv.at[l, :, pl.ds(i * head, head)], w_sem.at[l, i]) for i, w in enumerate((wq, wk, wv))]

    def gu_loads(l):
        cps = []
        for j in range(ff_tiles):
            n = min(head, ff - j * head)
            for i, w in enumerate((wg, wu)):
                cps.append(pltpu.make_async_copy(w.at[l, pl.ds(j * head, n)], wgu.at[l, pl.ds(j * TILE + i * head, n)], w_sem.at[l, 3 + 2 * j + i]))
        return cps

    def od_own(l):
        return [
            pltpu.make_async_copy(wo.at[l, :, my_cols], wod.at[l, k_rows(core, 0, head)], wo_sem.at[l, 0]),
            pltpu.make_async_copy(wd.at[l, :, my_cols], wod.at[l, k_rows(core, head, ff)], wo_sem.at[l, 1]),
        ]

    def od_partner(l):
        return [
            pltpu.make_async_remote_copy(wo.at[l, :, other_cols], wod.at[l, k_rows(core, 0, head)], wp_ssem.at[l, 0], wp_rsem.at[l, 0], device_id=partner),
            pltpu.make_async_remote_copy(wd.at[l, :, other_cols], wod.at[l, k_rows(core, head, ff)], wp_ssem.at[l, 1], wp_rsem.at[l, 1], device_id=partner),
        ]

    def cache_loads(l, b):
        span = pl.ds(b * rows * seq, rows * seq)
        return [
            pltpu.make_async_copy(kc.at[l, span], kbuf.at[b], c_sem.at[b, 0]),
            pltpu.make_async_copy(vc.at[l, span], vbuf.at[b], c_sem.at[b, 1]),
        ]

    def start(cps):
        for cp in cps:
            cp.start()

    def wait(cps):
        for cp in cps:
            cp.wait()

    start([x_load(0)])
    tail = ff - (ff_tiles - 1) * head
    for l in range(layers):
        for i in range(2):
            lo = (ff_tiles - 1) * TILE + i * head + tail // 16 * 16
            hi = (ff_tiles - 1) * TILE + (i + 1) * head
            wgu[l, lo:hi, :] = jnp.zeros((hi - lo, width), BF16)
            lo = i * kdim + (head + ff) // 16 * 16
            wod[l, lo:(i + 1) * kdim, :] = jnp.zeros(((i + 1) * kdim - lo, half), BF16)
    start(qkv_loads(0) + cache_loads(0, 0) + [x_load(1)] + gu_loads(0))
    bar = pltpu.get_barrier_semaphore()
    pl.semaphore_signal(bar, inc=1, device_id=partner)
    for k in range(1, chips):
        pl.semaphore_signal(bar, inc=1, device_id=dev(shift(py, k // side), shift(px, k % side), core))

    def norm_rows(b):
        def body(i, carry):
            y, x = lax.div(i, side), lax.rem(i, side)
            xv = out_ref[b, y, x].astype(F32)
            inv = lax.rsqrt(jnp.mean(xv * xv, axis=-1, keepdims=True) + NORM_EPS)
            a_buf[b, y, x] = (xv * inv * gain_ref[0]).astype(BF16)
            return carry
        lax.fori_loop(0, chips, body, 0, unroll=2)

    wait([x_load(0)])
    start(od_own(0))
    norm_rows(0)
    pl.semaphore_wait(bar, chips)
    start(od_partner(0))
    start(cache_loads(0, 1))
    for b in range(BLOCKS):
        start([pltpu.make_async_copy(x_hbm.at[b, py, px, :, my_cols], x_own.at[b], own_sem.at[b])])

    def compute(l, b):
        if b == 0:
            wait(qkv_loads(l))
        if l == 0 and b == 1:
            wait([x_load(1)])
            norm_rows(1)
        r0 = b * rows
        a = a_buf[b].reshape(rows, width)
        qkv = jnp.dot(a, wqkv[l], preferred_element_type=F32).astype(BF16)
        cosv, sinv = cos_ref[r0:r0 + rows, :], sin_ref[r0:r0 + rows, :]

        def rope(v):
            v = v.astype(F32)
            return (v * cosv + pltpu.roll(v, head // 2, 1) * sinv).astype(BF16)

        qr, kr = rope(qkv[:, :head]), rope(qkv[:, head:2 * head])
        q_s[...] = qr
        v_s[...] = qkv[:, 2 * head:]
        self_s[...] = jnp.sum(qr.astype(F32) * kr.astype(F32), axis=-1, keepdims=True) * scale
        yield
        if b == 0:
            wait(gu_loads(l))
        if l + b > 0:
            wait_send_h(b, l)
        for j in range(ff_tiles):
            gu = lax.dot_general(a_buf[b].reshape(rows, width), wgu[l, j * TILE:(j + 1) * TILE, :], NT, preferred_element_type=F32)
            gate = gu[:, :head].astype(BF16).astype(F32)
            up = gu[:, head:].astype(BF16).astype(F32)
            h_buf[b, core, :, (j + 1) * head:(j + 2) * head] = (gate * jax.nn.sigmoid(gate) * up).astype(BF16)
            yield
        wait(cache_loads(l, b))
        grp = 16
        row_id = lax.broadcasted_iota(jnp.int32, (grp, grp * seq), 0)
        dist = lax.broadcasted_iota(jnp.int32, (grp, grp * seq), 1) - row_id * seq

        def attend(g):
            sl = pl.ds(pl.multiple_of(g * grp, grp), grp)
            ks = pl.ds(pl.multiple_of(g * grp * seq, grp * seq), grp * seq)
            lens = len_ref[pl.ds(pl.multiple_of(r0 + g * grp, grp), grp), :]
            logits = lax.dot_general(q_s[sl, :], kbuf[b, ks, :], NT, preferred_element_type=F32) * scale
            logits = jnp.where((dist >= 0) & (dist < lens), logits, -jnp.inf)
            own = self_s[sl, :]
            peak = jnp.maximum(jnp.max(logits, axis=-1, keepdims=True), own)
            w = jnp.exp(logits - peak)
            own_w = jnp.exp(own - peak)
            inv = 1.0 / (jnp.sum(w, axis=-1, keepdims=True) + own_w)
            p = (w * inv).astype(BF16)
            own_p = (own_w * inv).astype(BF16).astype(F32)
            o = jnp.dot(p, vbuf[b, ks, :], preferred_element_type=F32) + own_p * v_s[sl, :].astype(F32)
            h_buf[b, core, sl, 0:head] = o.astype(BF16)

        unroll = 4

        def attend_some(i, carry):
            for u in range(unroll):
                attend(i * unroll + u)
            return carry

        lax.fori_loop(0, rows // grp // unroll, attend_some, 0)
        h_send(b).start()
        if l + 1 < layers:
            start(cache_loads(l + 1, b))
        yield
        if b == 0:
            wait(od_own(l))
            for cp in od_partner(l):
                cp.wait_recv()
        if l > 0:
            wait_send_rs(b)
        h_recv_wait(b)
        for j in range(half // TILE):
            cols = slice(j * TILE, (j + 1) * TILE)
            y = jnp.dot(h_buf[b, 0], wod[l, 0:kdim, cols], preferred_element_type=F32) + jnp.dot(h_buf[b, 1], wod[l, kdim:2 * kdim, cols], preferred_element_type=F32)
            send[b, :, :, :, cols] = y.astype(BF16).reshape(side, side, toks, TILE)
        for k in far_first:
            rs_copy(b, k).start()
        yield

    def h_send(b):
        return pltpu.make_async_remote_copy(h_buf.at[b, core], h_buf.at[b, core], h_ssem.at[b], h_rsem.at[b], device_id=partner)

    def h_recv_wait(b):
        wait_bytes(h_buf.at[b, other], h_rsem.at[b])

    def wait_send_h(b, l):
        if l > 0:
            wait_bytes(h_buf.at[b, core], h_ssem.at[b])

    def ring_dist(d):
        return min(d, side - d)

    far_first = sorted(range(1, chips), key=lambda k: -(ring_dist(k // side) + ring_dist(k % side)))

    def rs_copy(b, k):
        ty, tx = shift(py, k // side), shift(px, k % side)
        return pltpu.make_async_remote_copy(send.at[b, ty, tx], recv.at[b, k - 1], rs_ssem.at[b], rs_rsem.at[b], device_id=dev(ty, tx, core))

    def wait_send_rs(b):
        wait_bytes(recv.at[b], rs_ssem.at[b])

    def st_copy(b):
        return pltpu.make_async_remote_copy(st_send.at[b], st_recv.at[b], st_sem.at[b, 0], st_sem.at[b, 1], device_id=partner)

    def finish(l, b):
        last = l + 1 == layers
        buf = out_ref if last else a_buf
        if l == 0:
            wait_bytes(x_own.at[b], own_sem.at[b])
        wait_bytes(recv.at[b], rs_rsem.at[b])
        sq = jnp.zeros((toks, 128), F32)
        chunk = 256
        for c0 in range(0, half, chunk):
            cols = slice(c0, c0 + chunk)
            acc = send[b, py, px, :, cols].astype(F32)
            for k in range(chips - 1):
                acc = acc + recv[b, k, :, cols].astype(F32)
            xn = (x_own[b, :, cols].astype(F32) + acc).astype(BF16)
            if last:
                buf[b, py, px, :, pl.ds(pl.multiple_of(core * half + c0, chunk), chunk)] = xn
            else:
                x_own[b, :, cols] = xn
                xf = xn.astype(F32)
                for i in range(chunk // 128):
                    v = xf[:, i * 128:(i + 1) * 128]
                    sq = sq + v * v
        if not last:
            if l > 0:
                st_copy(b).wait_send()
            st_send[b] = sq
            st_copy(b).start()
            yield
            st_copy(b).wait_recv()
            total = jnp.sum(st_send[b] + st_recv[b], axis=-1, keepdims=True)
            inv = lax.rsqrt(total / width + NORM_EPS)
            for c0 in range(0, half, chunk):
                cc = pl.ds(pl.multiple_of(core * half + c0, chunk), chunk)
                buf[b, py, px, :, cc] = (x_own[b, :, c0:c0 + chunk].astype(F32) * inv * gain_ref[l + 1, :, cc]).astype(BF16)
        sgn = 1 - 2 * core

        def place(hf, p1, p2=None):
            first = slice(None) if p1 is None else p1
            y, x = (p2, first) if hf == 0 else (first, p2)
            return buf.at[b, y, x, :, part_cols(hf, core)]

        def pos(hf):
            return (px, py) if hf == 0 else (py, px)

        def at(hf, p1, p2):
            return dev(p2, p1, core) if hf == 0 else dev(p1, p2, core)

        def copy(hf, ref, target, idx):
            return pltpu.make_async_remote_copy(ref, ref, ag_ssem.at[b, hf, idx], ag_rsem.at[b, hf, idx], device_id=target)

        def to_partner(hf, ref, idx):
            return pltpu.make_async_remote_copy(ref, ref, d_ssem.at[b, hf, idx], d_rsem.at[b, hf, idx], device_id=partner)

        for idx, d in ((2, 2), (0, 1), (1, -1)):
            for hf in range(2):
                p1, p2 = pos(hf)
                copy(hf, place(hf, p1, p2), at(hf, shift(p1, d), p2), idx).start()
        yield
        for hf in range(2):
            p1, p2 = pos(hf)
            for idx, d in ((0, -1), (1, 1), (2, 2)):
                wait_bytes(place(hf, shift(p1, d), p2), ag_rsem.at[b, hf, idx])
            for idx, d in ((3, 1), (4, -1)):
                copy(hf, place(hf, None, p2), at(hf, p1, shift(p2, d)), idx).start()
            to_partner(hf, place(hf, None, p2), 0).start()
        yield
        for hf in range(2):
            p1, p2 = pos(hf)
            for near in (0, 1):
                pass
            src = shift(p2, -sgn)
            line = place(hf, None, src)
            wait_bytes(line, ag_rsem.at[b, hf, 3 + core])
            copy(hf, line, at(hf, p1, shift(p2, sgn)), 5).start()
            to_partner(hf, line, 1).start()
        yield
        for hf in range(2):
            p1, p2 = pos(hf)
            line = place(hf, None, shift(p2, sgn))
            wait_bytes(line, ag_rsem.at[b, hf, 4 - core])
            to_partner(hf, line, 2).start()
        yield
        for hf in range(2):
            p1, p2 = pos(hf)
            line = place(hf, None, shift(p2, 2))
            wait_bytes(line, ag_rsem.at[b, hf, 5])
            to_partner(hf, line, 3).start()
        yield
        for hf in range(2):
            p1, p2 = pos(hf)
            for idx in range(4):
                wait_bytes(place(hf, None, p2), d_rsem.at[b, hf, idx])
            for idx in range(3):
                wait_bytes(place(hf, p1, p2), ag_ssem.at[b, hf, idx])
            for idx in range(3, 6):
                wait_bytes(place(hf, None, p2), ag_ssem.at[b, hf, idx])
            for idx in range(4):
                wait_bytes(place(hf, None, p2), d_ssem.at[b, hf, idx])

    def run(gen):
        for _ in gen:
            pass

    def beside(main, background):
        for _ in main:
            next(background, None)
        run(background)

    run(compute(0, 0))
    start([cp for l in range(1, layers) for cp in qkv_loads(l) + gu_loads(l) + od_own(l) + od_partner(l)])
    run(compute(0, 1))
    for l in range(1, layers):
        run(finish(l - 1, 0))
        tail_gen = finish(l - 1, 1)
        next(tail_gen)
        next(tail_gen)
        beside(compute(l, 0), tail_gen)
        run(compute(l, 1))
    run(finish(layers - 1, 0))
    run(finish(layers - 1, 1))
    for l in range(layers):
        for cp in od_partner(l):
            cp.wait_send()
    for b in range(BLOCKS):
        wait_bytes(h_buf.at[b, core], h_ssem.at[b])
        wait_send_rs(b)
        if layers > 1:
            st_copy(b).wait_send()


def solution(mesh):
    tp_size = mesh.shape['tp']
    side = math.isqrt(tp_size // 2)
    arg_specs = (P('dp', None), P('dp'), P(), P(None, None, 'tp'), P(None, None, 'tp'), P(None, None, 'tp'), P(None, 'tp', None), P(None, None, 'tp'), P(None, None, 'tp'), P(None, 'tp', None), P(None, 'dp', None, 'tp', None), P(None, 'dp', None, 'tp', None))

    def per_device(x_in, lengths, norm_gain, w_q, w_k, w_v, w_o, w_gate, w_up, w_down, k_cache, v_cache):
        tok_rows, width = x_in.shape
        layers, _, head = w_q.shape
        ff = w_gate.shape[2]
        seq = k_cache.shape[2]
        chips = side * side
        rows = tok_rows // BLOCKS
        toks = rows // chips
        half = width // 2
        ff_tiles = -(-ff // head)
        kdim = head * (1 + ff_tiles)

        inv_freq = 1.0 / (ROPE_BASE ** (jnp.arange(0, head, 2).astype(F32) / head))
        angles = lengths.astype(F32)[:, None] * inv_freq[None, :]
        cos_ang, sin_ang = jnp.cos(angles), jnp.sin(angles)
        cos_full = jnp.concatenate([cos_ang, cos_ang], axis=-1)
        sin_full = jnp.concatenate([-sin_ang, sin_ang], axis=-1)

        any_spec = pl.BlockSpec(memory_space=pl.ANY)
        vmem_spec = pl.BlockSpec(memory_space=pltpu.VMEM)
        dma = pltpu.SemaphoreType.DMA
        out = pl.pallas_call(
            functools.partial(layers_kernel, side),
            out_shape=jax.ShapeDtypeStruct((BLOCKS, side, side, toks, width), BF16),
            in_specs=[any_spec] + [vmem_spec] * 4 + [any_spec] * 9,
            out_specs=vmem_spec,
            scratch_shapes=[
                pltpu.VMEM((BLOCKS, side, side, toks, width), BF16),
                pltpu.VMEM((layers, width, 3 * head), BF16),
                pltpu.VMEM((layers, ff_tiles * TILE, width), BF16),
                pltpu.VMEM((layers, 2 * kdim, half), BF16),
                pltpu.VMEM((BLOCKS, rows * seq, head), BF16),
                pltpu.VMEM((BLOCKS, rows * seq, head), BF16),
                pltpu.VMEM((rows, head), BF16),
                pltpu.VMEM((rows, head), BF16),
                pltpu.VMEM((rows, head), BF16),
                pltpu.VMEM((rows, 1), F32),
                pltpu.VMEM((BLOCKS, 2, rows, kdim), BF16),
                pltpu.VMEM((BLOCKS, side, side, toks, half), BF16),
                pltpu.VMEM((BLOCKS, chips - 1, toks, half), BF16),
                pltpu.VMEM((BLOCKS, toks, half), BF16),
                pltpu.VMEM((BLOCKS, toks, 128), F32),
                pltpu.VMEM((BLOCKS, toks, 128), F32),
                dma((BLOCKS,)),
                dma((layers, 3 + 2 * ff_tiles)),
                dma((layers, 2)),
                dma((layers, 2)),
                dma((layers, 2)),
                dma((BLOCKS, 2)),
                dma((BLOCKS,)),
                dma((BLOCKS,)),
                dma((BLOCKS,)),
                dma((BLOCKS,)),
                dma((BLOCKS,)),
                dma((BLOCKS, 2)),
                dma((BLOCKS, 2, 6)),
                dma((BLOCKS, 2, 6)),
                dma((BLOCKS, 2, 4)),
                dma((BLOCKS, 2, 4)),
            ],
            compiler_params=pltpu.CompilerParams(collective_id=0, has_side_effects=True, vmem_limit_bytes=67043328),
            name='decoder_layers',
        )(
            x_in.reshape(BLOCKS, side, side, toks, width),
            lengths.reshape(tok_rows, 1),
            cos_full,
            sin_full,
            norm_gain.astype(F32).reshape(layers, 1, width),
            w_q, w_k, w_v, w_o,
            w_gate.swapaxes(1, 2),
            w_up.swapaxes(1, 2),
            w_down,
            k_cache.reshape(layers, tok_rows * seq, head),
            v_cache.reshape(layers, tok_rows * seq, head),
        )
        return out.reshape(tok_rows, width)

    return jax.shard_map(per_device, mesh=mesh, in_specs=arg_specs, out_specs=P('dp', None), check_vma=False)
```

```python
import functools
import math

import jax
import jax.numpy as jnp
import numpy as np
from jax import lax
from jax.experimental import pallas as pl
from jax.experimental.pallas import tpu as pltpu
from jax.sharding import PartitionSpec as P

NORM_EPS = 1e-5
ROPE_BASE = 500000.0
F32 = jnp.float32
BF16 = jnp.bfloat16
NT = (((1,), (1,)), ((), ()))
BLOCKS = 2
TILE = 256


def wait_bytes(ref, sem):
    pltpu.make_async_copy(ref, ref, sem).wait()


def layers_kernel(side, x_hbm, len_hbm, freq_hbm, gain_hbm, wq, wk, wv, wo, wg, wu, wd, kc, vc, out_hbm,
                  len_in, freq_ref, gain_ref, out_ref, len_ref, cos_ref, sin_ref, lg_s, pr_s, ow_s, a_buf, wqkv, wgu, wod, kbuf, vbuf, q_s, v_s, self_s, h_buf, send, r1, mid, r2, x_own, st_send, st_recv,
                  small_sem, x_sem, w_sem, wo_sem, wp_ssem, wp_rsem, c_sem, own_sem, h_ssem, h_rsem, p1_ssem, p1_rsem, p2_ssem, p2_rsem, st_sem, ag_ssem, ag_rsem, d_ssem, d_rsem, out_sem):
    layers, width = wq.shape[0], wq.shape[1]
    head = wq.shape[2]
    ff = wd.shape[1]
    half = width // 2
    quarter = width // 4
    toks = x_hbm.shape[3]
    chips = side * side
    rows = chips * toks
    seq = kc.shape[1] // (BLOCKS * rows)
    ff_tiles = wgu.shape[1] // TILE
    kdim = h_buf.shape[3]
    scale = head ** -0.5

    me = lax.axis_index('tp')
    core = lax.rem(me, 2)
    chip = lax.div(me, 2)
    px = lax.rem(chip, side)
    py = lax.div(chip, side)
    other = 1 - core

    def dev(y, x, c):
        return {'tp': (y * side + x) * 2 + c}

    def shift(p, d):
        return lax.rem(p + d + side, side)

    partner = dev(py, px, other)
    my_cols = pl.ds(pl.multiple_of(core * half, half), half)
    other_cols = pl.ds(pl.multiple_of(other * half, half), half)

    def part_cols(hf, c):
        return pl.ds(pl.multiple_of(c * half + hf * quarter, quarter), quarter)

    def k_rows(c, start, n):
        return pl.ds(pl.multiple_of(c * kdim + start, 8), n)

    def x_load(b):
        return pltpu.make_async_copy(x_hbm.at[b], out_ref.at[b], x_sem.at[b])

    def qkv_loads(l):
        return [pltpu.make_async_copy(w.at[l], wqkv.at[l, :, pl.ds(i * head, head)], w_sem.at[l, i]) for i, w in enumerate((wq, wk, wv))]

    def gu_loads(l):
        cps = []
        for j in range(ff_tiles):
            n = min(head, ff - j * head)
            for i, w in enumerate((wg, wu)):
                cps.append(pltpu.make_async_copy(w.at[l, pl.ds(j * head, n)], wgu.at[l, pl.ds(j * TILE + i * head, n)], w_sem.at[l, 3 + 2 * j + i]))
        return cps

    def od_own(l):
        return [
            pltpu.make_async_copy(wo.at[l, :, my_cols], wod.at[l, k_rows(core, 0, head)], wo_sem.at[l, 0]),
            pltpu.make_async_copy(wd.at[l, :, my_cols], wod.at[l, k_rows(core, head, ff)], wo_sem.at[l, 1]),
        ]

    def od_partner(l):
        return [
            pltpu.make_async_remote_copy(wo.at[l, :, other_cols], wod.at[l, k_rows(core, 0, head)], wp_ssem.at[l, 0], wp_rsem.at[l, 0], device_id=partner),
            pltpu.make_async_remote_copy(wd.at[l, :, other_cols], wod.at[l, k_rows(core, head, ff)], wp_ssem.at[l, 1], wp_rsem.at[l, 1], device_id=partner),
        ]

    def cache_loads(l, b):
        span = pl.ds(b * rows * seq, rows * seq)
        return [
            pltpu.make_async_copy(kc.at[l, span], kbuf.at[b], c_sem.at[b, 0]),
            pltpu.make_async_copy(vc.at[l, span], vbuf.at[b], c_sem.at[b, 1]),
        ]

    def start(cps):
        for cp in cps:
            cp.start()

    def wait(cps):
        for cp in cps:
            cp.wait()

    smalls = [pltpu.make_async_copy(src, dst, small_sem.at[i]) for i, (src, dst) in enumerate(((gain_hbm, gain_ref), (len_hbm, len_in), (freq_hbm, freq_ref)))]
    start(smalls + [x_load(0)] + qkv_loads(0))
    bar = pltpu.get_barrier_semaphore()

    def norm_rows(b):
        def body(i, carry):
            y, x = lax.div(i, side), lax.rem(i, side)
            xv = out_ref[b, y, x].astype(F32)
            inv = lax.rsqrt(jnp.mean(xv * xv, axis=-1, keepdims=True) + NORM_EPS)
            a_buf[b, y, x] = (xv * inv * gain_ref[0:1, :].astype(F32)).astype(BF16)
            return carry
        lax.fori_loop(0, chips, body, 0, unroll=2)

    tail = ff - (ff_tiles - 1) * head
    with jax.named_scope('zeros'):
        for l in range(layers):
            for i in range(2):
                lo = (ff_tiles - 1) * TILE + i * head + tail // 16 * 16
                hi = (ff_tiles - 1) * TILE + (i + 1) * head
                wgu[l, lo:hi, :] = jnp.zeros((hi - lo, width), BF16)
                lo = i * kdim + (head + ff) // 16 * 16
                wod[l, lo:(i + 1) * kdim, :] = jnp.zeros(((i + 1) * kdim - lo, half), BF16)
    pl.semaphore_signal(bar, inc=1, device_id=partner)
    for k in range(1, chips):
        pl.semaphore_signal(bar, inc=1, device_id=dev(shift(py, k // side), shift(px, k % side), core))
    with jax.named_scope('wait_x'):
        wait(smalls + [x_load(0)])
    start(gu_loads(0) + cache_loads(0, 0) + od_own(0))
    with jax.named_scope('norm_00'):
        norm_rows(0)
    with jax.named_scope('tables'):
        lane = lax.broadcasted_iota(jnp.int32, (128, head), 1)
        for i in range(len_in.shape[0]):
            pos_rows = jnp.broadcast_to(len_in[i:i + 1, :].astype(F32), (128, 128)).T
            len_ref[i * 128:(i + 1) * 128, :] = pos_rows[:, 0:1].astype(jnp.int32)
            angle = pos_rows[:, 0:head] * freq_ref[...]
            cos_ref[i * 128:(i + 1) * 128, :] = jnp.cos(angle)
            sin = jnp.sin(angle)
            sin_ref[i * 128:(i + 1) * 128, :] = jnp.where(lane < head // 2, -sin, sin)

    def enter():
        with jax.named_scope('barrier'):
            pl.semaphore_wait(bar, chips)
        start(od_partner(0))
        for l in range(1, layers):
            start(qkv_loads(l) + gu_loads(l) + od_own(l) + od_partner(l))

    for b in range(1, BLOCKS):
        start([x_load(b)] + cache_loads(0, b))
    for b in range(BLOCKS):
        start([pltpu.make_async_copy(x_hbm.at[b, py, px, :, my_cols], x_own.at[b], own_sem.at[b])])

    part = rows / 256

    def chain(b):
        for l in range(layers):
            yield from compute(l, b)
            yield from finish(l, b)

    def compute(l, b):
        if b == 0:
            with jax.named_scope(f'wait_qkv_{l}{b}'):
                wait(qkv_loads(l))
        if l == 0 and b > 0:
            with jax.named_scope(f'norm_{l}{b}'):
                wait([x_load(b)])
                norm_rows(b)
        r0 = b * rows
        with jax.named_scope(f'qkv_{l}{b}'):
            a = a_buf[b].reshape(rows, width)
            qkv = jnp.dot(a, wqkv[l], preferred_element_type=F32).astype(BF16)
            cosv, sinv = cos_ref[r0:r0 + rows, :], sin_ref[r0:r0 + rows, :]

            def rope(v):
                v = v.astype(F32)
                return (v * cosv + pltpu.roll(v, head // 2, 1) * sinv).astype(BF16)

            qr, kr = rope(qkv[:, :head]), rope(qkv[:, head:2 * head])
            q_s[b] = qr
            v_s[b] = qkv[:, 2 * head:]
            self_s[b] = jnp.sum(qr.astype(F32) * kr.astype(F32), axis=-1, keepdims=True) * scale
        yield 1.5 * part + (1.5 * part if l == 0 else 0), 0, 0, False
        if l == 0 and b == 0:
            enter()
        with jax.named_scope(f'wait_gu_{l}{b}'):
            if b == 0:
                wait(gu_loads(l))
        if l > 0:
            for i in range(2):
                h_send(b, i).wait_send()
        for j in range(ff_tiles):
            with jax.named_scope(f'gu_{l}{b}'):
                gu = lax.dot_general(a_buf[b].reshape(rows, width), wgu[l, j * TILE:(j + 1) * TILE, :], NT, preferred_element_type=F32)
                gate = gu[:, :head].astype(BF16).astype(F32)
                up = gu[:, head:].astype(BF16).astype(F32)
                h_buf[b, core, :, (j + 1) * head:(j + 2) * head] = (gate * jax.nn.sigmoid(gate) * up).astype(BF16)
            if j + 1 == ff_tiles:
                h_send(b, 1).start()
            yield 0.8 * part, 0, 0, False
        with jax.named_scope(f'wait_cache_{l}{b}'):
            wait(cache_loads(l, b))
        grp = 16
        unroll = 4
        span = 64

        def group(g):
            return pl.ds(pl.multiple_of(g * grp, grp), grp), pl.ds(pl.multiple_of(g * grp * seq, grp * seq), grp * seq)

        def score(i, carry):
            for u in range(unroll):
                sl, ks = group(i * unroll + u)
                lg_s[b, sl, :] = lax.dot_general(q_s[b, sl, :], kbuf[b, ks, :], NT, preferred_element_type=F32)
            return carry

        def soften(i, carry):
            sl = pl.ds(pl.multiple_of(i * span, span), span)
            lens = len_ref[pl.ds(pl.multiple_of(r0 + i * span, span), span), :]
            row_id = lax.rem(lax.broadcasted_iota(jnp.int32, (span, grp * seq), 0), grp)
            dist = lax.broadcasted_iota(jnp.int32, (span, grp * seq), 1) - row_id * seq
            logits = jnp.where((dist >= 0) & (dist < lens), lg_s[b, sl, :] * scale, -jnp.inf)
            own = self_s[b, sl, :]
            peak = jnp.maximum(jnp.max(logits, axis=-1, keepdims=True), own)
            w = jnp.exp(logits - peak)
            own_w = jnp.exp(own - peak)
            inv = 1.0 / (jnp.sum(w, axis=-1, keepdims=True) + own_w)
            pr_s[b, sl, :] = (w * inv).astype(BF16)
            ow_s[b, sl, :] = (own_w * inv).astype(BF16).astype(F32)
            return carry

        def mix(i, carry):
            for u in range(unroll):
                sl, ks = group(i * unroll + u)
                o = jnp.dot(pr_s[b, sl, :], vbuf[b, ks, :], preferred_element_type=F32) + ow_s[b, sl, :] * v_s[b, sl, :].astype(F32)
                h_buf[b, core, sl, 0:head] = o.astype(BF16)
            return carry

        with jax.named_scope(f'score_{l}{b}'):
            lax.fori_loop(0, rows // grp // unroll, score, 0)
        with jax.named_scope(f'soften_{l}{b}'):
            lax.fori_loop(0, rows // span, soften, 0)
        with jax.named_scope(f'mix_{l}{b}'):
            lax.fori_loop(0, rows // grp // unroll, mix, 0)
        h_send(b, 0).start()
        if l + 1 < layers:
            start(cache_loads(l + 1, b))
        yield 3.4 * part, 0, 1.5, False
        with jax.named_scope(f'wait_down_{l}{b}'):
            if b == 0:
                wait(od_own(l))
                for cp in od_partner(l):
                    cp.wait_recv()
            for i in range(2):
                h_send(b, i).wait_recv()
        for hf in range(2):
            with jax.named_scope(f'down_{l}{b}'):
                if l > 0:
                    for k in range(1, side):
                        p1_copy(b, hf, k).wait_send()
                for j in range(hf * quarter // TILE, (hf + 1) * quarter // TILE):
                    cols = slice(j * TILE, (j + 1) * TILE)
                    y = jnp.dot(h_buf[b, 0], wod[l, 0:kdim, cols], preferred_element_type=F32) + jnp.dot(h_buf[b, 1], wod[l, kdim:2 * kdim, cols], preferred_element_type=F32)
                    send[b, :, :, :, cols] = y.astype(BF16).reshape(side, side, toks, TILE)
                for k in far_first:
                    p1_copy(b, hf, k).start()
        yield 1.8 * part, 5.6 * part, 2.2, True

    def h_send(b, i):
        ref = h_buf.at[b, core, :, pl.ds(0, head)] if i == 0 else h_buf.at[b, core, :, pl.ds(head, kdim - head)]
        return pltpu.make_async_remote_copy(ref, ref, h_ssem.at[b, i], h_rsem.at[b, i], device_id=partner)

    far_first = sorted(range(1, side), key=lambda k: -min(k, side - k))

    def pos(hf):
        return (px, py) if hf == 0 else (py, px)

    def at(hf, p1, p2):
        return dev(p2, p1, core) if hf == 0 else dev(p1, p2, core)

    def line_of(ref, b, hf, p1, cols):
        return ref.at[b, :, p1, :, cols] if hf == 0 else ref.at[b, p1, :, :, cols]

    def hf_cols(hf):
        return pl.ds(hf * quarter, quarter)

    def p1_copy(b, hf, k):
        p1, p2 = pos(hf)
        to = shift(p1, k)
        return pltpu.make_async_remote_copy(line_of(send, b, hf, to, hf_cols(hf)), r1.at[b, hf, k - 1], p1_ssem.at[b, hf, k - 1], p1_rsem.at[b, hf, k - 1], device_id=at(hf, to, p2))

    def p2_copy(b, hf, k):
        p1, p2 = pos(hf)
        to = shift(p2, k)
        return pltpu.make_async_remote_copy(mid.at[b, hf, to], r2.at[b, hf, k - 1], p2_ssem.at[b, hf, k - 1], p2_rsem.at[b, hf, k - 1], device_id=at(hf, p1, to))

    def st_copy(b):
        return pltpu.make_async_remote_copy(st_send.at[b], st_recv.at[b], st_sem.at[b, 0], st_sem.at[b, 1], device_id=partner)

    def finish(l, b):
        last = l + 1 == layers
        buf = out_ref if last else a_buf
        if l == 0:
            wait_bytes(x_own.at[b], own_sem.at[b])
        chunk = 256
        for hf in range(2):
            p1, p2 = pos(hf)
            with jax.named_scope(f'wait_p1_{l}{b}'):
                for k in range(1, side):
                    p1_copy(b, hf, k).wait_recv()
                    if l > 0:
                        p2_copy(b, hf, k).wait_send()
            with jax.named_scope(f'mid_{l}{b}'):
                for q in range(side):
                    own = send[b, q, p1, :, hf * quarter:(hf + 1) * quarter] if hf == 0 else send[b, p1, q, :, hf * quarter:(hf + 1) * quarter]
                    acc = own.astype(F32)
                    for k in range(side - 1):
                        acc = acc + r1[b, hf, k, q].astype(F32)
                    mid[b, hf, q] = acc
                for k in far_first:
                    p2_copy(b, hf, k).start()
        yield 0.4 * part, 2.8 * part, 2.2, True
        sq = jnp.zeros((toks, 128), F32)
        for hf in range(2):
            p1, p2 = pos(hf)
            with jax.named_scope(f'wait_p2_{l}{b}'):
                for k in range(1, side):
                    p2_copy(b, hf, k).wait_recv()
            with jax.named_scope(f'reduce_{l}{b}'):
                for c0 in range(0, quarter, chunk):
                    cols = slice(c0, c0 + chunk)
                    xc = slice(hf * quarter + c0, hf * quarter + c0 + chunk)
                    acc = mid[b, hf, p2, :, cols]
                    for k in range(side - 1):
                        acc = acc + r2[b, hf, k, :, cols]
                    xn = (x_own[b, :, xc].astype(F32) + acc).astype(BF16)
                    if last:
                        buf[b, py, px, :, pl.ds(pl.multiple_of(core * half + hf * quarter + c0, chunk), chunk)] = xn
                    else:
                        x_own[b, :, xc] = xn
                        xf = xn.astype(F32)
                        for i in range(chunk // 128):
                            v = xf[:, i * 128:(i + 1) * 128]
                            sq = sq + v * v
        if not last:
            if l > 0:
                st_copy(b).wait_send()
            st_send[b] = sq
            st_copy(b).start()
            yield 0.2 * part, 0, 1.4, True
            with jax.named_scope(f'wait_st_{l}{b}'):
                st_copy(b).wait_recv()
            with jax.named_scope(f'scale_{l}{b}'):
                total = jnp.sum(st_send[b] + st_recv[b], axis=-1, keepdims=True)
                inv = lax.rsqrt(total / width + NORM_EPS)
                for c0 in range(0, half, chunk):
                    cc = pl.ds(pl.multiple_of(core * half + c0, chunk), chunk)
                    buf[b, py, px, :, cc] = (x_own[b, :, c0:c0 + chunk].astype(F32) * inv * gain_ref[l + 1:l + 2, cc].astype(F32)).astype(BF16)
        sgn = 1 - 2 * core

        def place(hf, p1, p2=None):
            first = slice(None) if p1 is None else p1
            y, x = (p2, first) if hf == 0 else (first, p2)
            return buf.at[b, y, x, :, part_cols(hf, core)]

        def copy(hf, ref, target, idx):
            return pltpu.make_async_remote_copy(ref, ref, ag_ssem.at[b, hf, idx], ag_rsem.at[b, hf, idx], device_id=target)

        def place_out(hf, c, p2, idx):
            y, x = (p2, slice(None)) if hf == 0 else (slice(None), p2)
            cols = part_cols(hf, c)
            return pltpu.make_async_copy(buf.at[b, y, x, :, cols], out_hbm.at[b, y, x, :, cols], out_sem.at[b, hf, idx])

        def to_partner(hf, ref, idx):
            return pltpu.make_async_remote_copy(ref, ref, d_ssem.at[b, hf, idx], d_rsem.at[b, hf, idx], device_id=partner)

        for idx, d in ((2, 2), (0, 1), (1, -1)):
            for hf in range(2):
                p1, p2 = pos(hf)
                copy(hf, place(hf, p1, p2), at(hf, shift(p1, d), p2), idx).start()
        yield 0.2, 1.4 * part, 2.6, True
        with jax.named_scope(f'gather1_{l}{b}'):
            for hf in range(2):
                p1, p2 = pos(hf)
                for idx, d in ((0, -1), (1, 1), (2, 2)):
                    wait_bytes(place(hf, shift(p1, d), p2), ag_rsem.at[b, hf, idx])
                for idx, d in ((3, 1), (4, -1)):
                    copy(hf, place(hf, None, p2), at(hf, p1, shift(p2, d)), idx).start()
                to_partner(hf, place(hf, None, p2), 0).start()
                if last:
                    place_out(hf, core, p2, 0).start()
        yield 0.1, 2.8 * part, 2.2, True
        with jax.named_scope(f'gather2_{l}{b}'):
            for hf in range(2):
                p1, p2 = pos(hf)
                src = shift(p2, -sgn)
                line = place(hf, None, src)
                wait_bytes(line, ag_rsem.at[b, hf, 3 + core])
                copy(hf, line, at(hf, p1, shift(p2, sgn)), 5).start()
                to_partner(hf, line, 1).start()
                if last:
                    place_out(hf, core, src, 1).start()
        yield 0.1, 1.4 * part, 0, True
        with jax.named_scope(f'gather3_{l}{b}'):
            for hf in range(2):
                p1, p2 = pos(hf)
                line = place(hf, None, shift(p2, sgn))
                wait_bytes(line, ag_rsem.at[b, hf, 4 - core])
                to_partner(hf, line, 2).start()
                if last:
                    place_out(hf, core, shift(p2, sgn), 2).start()
        yield 0, 0, 2.2, True
        with jax.named_scope(f'gather4_{l}{b}'):
            for hf in range(2):
                p1, p2 = pos(hf)
                line = place(hf, None, shift(p2, 2))
                wait_bytes(line, ag_rsem.at[b, hf, 5])
                to_partner(hf, line, 3).start()
                if last:
                    place_out(hf, core, shift(p2, 2), 3).start()
        yield 0, 0, 1.2, True
        with jax.named_scope(f'gather5_{l}{b}'):
            for hf in range(2):
                p1, p2 = pos(hf)
                for idx, d in enumerate((0, sgn, -sgn, 2)):
                    wait_bytes(place(hf, None, p2), d_rsem.at[b, hf, idx])
                    if last:
                        place_out(hf, other, shift(p2, d), 4 + idx).start()
                for idx in range(3):
                    wait_bytes(place(hf, p1, p2), ag_ssem.at[b, hf, idx])
                for idx in range(3, 6):
                    wait_bytes(place(hf, None, p2), ag_ssem.at[b, hf, idx])
                for idx in range(4):
                    wait_bytes(place(hf, None, p2), d_ssem.at[b, hf, idx])
        if last:
            finals.append(lambda: [place_out(hf, core, shift(pos(hf)[1], 0), idx).wait() for hf in range(2) for idx in range(8)])

    finals = []

    chains = {b: chain(b) for b in range(BLOCKS)}
    ready, light = [0.0] * BLOCKS, [False] * BLOCKS
    now = free = 0.0
    turn = [0, 0]
    while chains:
        if turn:
            b = turn.pop()
        else:
            b = min(chains, key=lambda c: (max(ready[c], now), not light[c], c))
        step = next(chains[b], None)
        if step is None:
            del chains[b]
            continue
        spent, link, delay, light[b] = step
        now = max(now, ready[b]) + spent
        if link:
            free = max(free, now) + link
            ready[b] = free + delay
        else:
            ready[b] = now + delay
    for fin in finals:
        fin()
    for l in range(layers):
        for cp in od_partner(l):
            cp.wait_send()
    for b in range(BLOCKS):
        for i in range(2):
            h_send(b, i).wait_send()
            for k in range(1, side):
                p1_copy(b, i, k).wait_send()
                p2_copy(b, i, k).wait_send()
        if layers > 1:
            st_copy(b).wait_send()


def solution(mesh):
    tp_size = mesh.shape['tp']
    side = math.isqrt(tp_size // 2)
    arg_specs = (P('dp', None), P('dp'), P(), P(None, None, 'tp'), P(None, None, 'tp'), P(None, None, 'tp'), P(None, 'tp', None), P(None, None, 'tp'), P(None, None, 'tp'), P(None, 'tp', None), P(None, 'dp', None, 'tp', None), P(None, 'dp', None, 'tp', None))

    def per_device(x_in, lengths, norm_gain, w_q, w_k, w_v, w_o, w_gate, w_up, w_down, k_cache, v_cache):
        tok_rows, width = x_in.shape
        layers, _, head = w_q.shape
        ff = w_gate.shape[2]
        seq = k_cache.shape[2]
        chips = side * side
        rows = tok_rows // BLOCKS
        toks = rows // chips
        half = width // 2
        ff_tiles = -(-ff // head)
        kdim = head * (1 + ff_tiles)

        inv_freq = (1.0 / (ROPE_BASE ** (np.arange(0, head, 2, dtype=np.float64) / head))).astype(np.float32)
        freq = jnp.asarray(np.concatenate([inv_freq, inv_freq])[None, :])

        any_spec = pl.BlockSpec(memory_space=pl.ANY)
        dma = pltpu.SemaphoreType.DMA
        out = pl.pallas_call(
            functools.partial(layers_kernel, side),
            out_shape=jax.ShapeDtypeStruct((BLOCKS, side, side, toks, width), BF16),
            in_specs=[any_spec] * 13,
            out_specs=any_spec,
            scratch_shapes=[
                pltpu.VMEM((tok_rows // 128, 128), jnp.int32),
                pltpu.VMEM((1, head), F32),
                pltpu.VMEM((layers, width), BF16),
                pltpu.VMEM((BLOCKS, side, side, toks, width), BF16),
                pltpu.VMEM((tok_rows, 1), jnp.int32),
                pltpu.VMEM((tok_rows, head), F32),
                pltpu.VMEM((tok_rows, head), F32),
                pltpu.VMEM((BLOCKS, rows, 16 * seq), F32),
                pltpu.VMEM((BLOCKS, rows, 16 * seq), BF16),
                pltpu.VMEM((BLOCKS, rows, 1), F32),
                pltpu.VMEM((BLOCKS, side, side, toks, width), BF16),
                pltpu.VMEM((layers, width, 3 * head), BF16),
                pltpu.VMEM((layers, ff_tiles * TILE, width), BF16),
                pltpu.VMEM((layers, 2 * kdim, half), BF16),
                pltpu.VMEM((BLOCKS, rows * seq, head), BF16),
                pltpu.VMEM((BLOCKS, rows * seq, head), BF16),
                pltpu.VMEM((BLOCKS, rows, head), BF16),
                pltpu.VMEM((BLOCKS, rows, head), BF16),
                pltpu.VMEM((BLOCKS, rows, 1), F32),
                pltpu.VMEM((BLOCKS, 2, rows, kdim), BF16),
                pltpu.VMEM((BLOCKS, side, side, toks, half), BF16),
                pltpu.VMEM((BLOCKS, 2, side - 1, side, toks, half // 2), BF16),
                pltpu.VMEM((BLOCKS, 2, side, toks, half // 2), F32),
                pltpu.VMEM((BLOCKS, 2, side - 1, toks, half // 2), F32),
                pltpu.VMEM((BLOCKS, toks, half), BF16),
                pltpu.VMEM((BLOCKS, toks, 128), F32),
                pltpu.VMEM((BLOCKS, toks, 128), F32),
                dma((3,)),
                dma((BLOCKS,)),
                dma((layers, 3 + 2 * ff_tiles)),
                dma((layers, 2)),
                dma((layers, 2)),
                dma((layers, 2)),
                dma((BLOCKS, 2)),
                dma((BLOCKS,)),
                dma((BLOCKS, 2)),
                dma((BLOCKS, 2)),
                dma((BLOCKS, 2, side - 1)),
                dma((BLOCKS, 2, side - 1)),
                dma((BLOCKS, 2, side - 1)),
                dma((BLOCKS, 2, side - 1)),
                dma((BLOCKS, 2)),
                dma((BLOCKS, 2, 6)),
                dma((BLOCKS, 2, 6)),
                dma((BLOCKS, 2, 4)),
                dma((BLOCKS, 2, 4)),
                dma((BLOCKS, 2, 8)),
            ],
            compiler_params=pltpu.CompilerParams(collective_id=0, has_side_effects=True, vmem_limit_bytes=67043328),
            name='decoder_layers',
        )(
            x_in.reshape(BLOCKS, side, side, toks, width),
            lengths.reshape(tok_rows // 128, 128),
            freq,
            norm_gain,
            w_q, w_k, w_v, w_o,
            w_gate.swapaxes(1, 2),
            w_up.swapaxes(1, 2),
            w_down,
            k_cache.reshape(layers, tok_rows * seq, head),
            v_cache.reshape(layers, tok_rows * seq, head),
        )
        return out.reshape(tok_rows, width)

    return jax.shard_map(per_device, mesh=mesh, in_specs=arg_specs, out_specs=P('dp', None), check_vma=False)
```

```python
import functools
import math

import jax
import jax.numpy as jnp
import numpy as np
from jax import lax
from jax.experimental import pallas as pl
from jax.experimental.pallas import tpu as pltpu
from jax.sharding import PartitionSpec as P

NORM_EPS = 1e-5
ROPE_BASE = 500000.0
F32 = jnp.float32
BF16 = jnp.bfloat16
NT = (((1,), (1,)), ((), ()))
BLOCKS = 2
WIRE = 1.0
TILE = 256


def wait_bytes(ref, sem):
    pltpu.make_async_copy(ref, ref, sem).wait()


def layers_kernel(side, x_hbm, len_hbm, freq_hbm, gain_hbm, wq, wk, wv, wo, wg, wu, wd, kc, vc, out_ref,
                  len_in, freq_ref, gain_ref, len_ref, cos_ref, sin_ref, lg_s, pr_s, ow_s, a_buf, wqkv, wgu, wod, kbuf, vbuf, q_s, v_s, self_s, h_buf, send, r1, mid, r2, x_own, st_send, st_recv,
                  small_sem, x_sem, w_sem, wo_sem, wp_ssem, wp_rsem, c_sem, own_sem, h_ssem, h_rsem, p1_ssem, p1_rsem, p2_ssem, p2_rsem, st_sem, ag_ssem, ag_rsem, d_ssem, d_rsem):
    layers, width = wq.shape[0], wq.shape[1]
    head = wq.shape[2]
    ff = wd.shape[1]
    half = width // 2
    quarter = width // 4
    toks = x_hbm.shape[3]
    chips = side * side
    rows = chips * toks
    seq = kc.shape[1] // (BLOCKS * rows)
    ff_tiles = wgu.shape[1] // TILE
    kdim = h_buf.shape[3]
    scale = head ** -0.5

    me = lax.axis_index('tp')
    core = lax.rem(me, 2)
    chip = lax.div(me, 2)
    px = lax.rem(chip, side)
    py = lax.div(chip, side)
    other = 1 - core

    def dev(y, x, c):
        return {'tp': (y * side + x) * 2 + c}

    def shift(p, d):
        return lax.rem(p + d + side, side)

    partner = dev(py, px, other)
    my_cols = pl.ds(pl.multiple_of(core * half, half), half)
    other_cols = pl.ds(pl.multiple_of(other * half, half), half)

    def part_cols(hf, c):
        return pl.ds(pl.multiple_of(c * half + hf * quarter, quarter), quarter)

    def k_rows(c, start, n):
        return pl.ds(pl.multiple_of(c * kdim + start, 8), n)

    def x_load(b):
        return pltpu.make_async_copy(x_hbm.at[b], out_ref.at[b], x_sem.at[b])

    def qkv_loads(l):
        return [pltpu.make_async_copy(w.at[l], wqkv.at[l, :, pl.ds(i * head, head)], w_sem.at[l, i]) for i, w in enumerate((wq, wk, wv))]

    def gu_loads(l):
        cps = []
        for j in range(ff_tiles):
            n = min(head, ff - j * head)
            for i, w in enumerate((wg, wu)):
                cps.append(pltpu.make_async_copy(w.at[l, pl.ds(j * head, n)], wgu.at[l, pl.ds(j * TILE + i * head, n)], w_sem.at[l, 3 + 2 * j + i]))
        return cps

    def od_own(l):
        return [
            pltpu.make_async_copy(wo.at[l, :, my_cols], wod.at[l, k_rows(core, 0, head)], wo_sem.at[l, 0]),
            pltpu.make_async_copy(wd.at[l, :, my_cols], wod.at[l, k_rows(core, head, ff)], wo_sem.at[l, 1]),
        ]

    def od_partner(l):
        return [
            pltpu.make_async_remote_copy(wo.at[l, :, other_cols], wod.at[l, k_rows(core, 0, head)], wp_ssem.at[l, 0], wp_rsem.at[l, 0], device_id=partner),
            pltpu.make_async_remote_copy(wd.at[l, :, other_cols], wod.at[l, k_rows(core, head, ff)], wp_ssem.at[l, 1], wp_rsem.at[l, 1], device_id=partner),
        ]

    def cache_loads(l, b):
        span = pl.ds(b * rows * seq, rows * seq)
        return [
            pltpu.make_async_copy(kc.at[l, span], kbuf.at[b], c_sem.at[b, 0]),
            pltpu.make_async_copy(vc.at[l, span], vbuf.at[b], c_sem.at[b, 1]),
        ]

    def start(cps):
        for cp in cps:
            cp.start()

    def wait(cps):
        for cp in cps:
            cp.wait()

    smalls = [pltpu.make_async_copy(src, dst, small_sem.at[i]) for i, (src, dst) in enumerate(((gain_hbm, gain_ref), (len_hbm, len_in), (freq_hbm, freq_ref)))]
    start(smalls + [x_load(0)] + qkv_loads(0))
    bar = pltpu.get_barrier_semaphore()

    def norm_rows(b):
        def body(i, carry):
            y, x = lax.div(i, side), lax.rem(i, side)
            xv = out_ref[b, y, x].astype(F32)
            inv = lax.rsqrt(jnp.mean(xv * xv, axis=-1, keepdims=True) + NORM_EPS)
            a_buf[b, y, x] = (xv * inv * gain_ref[0:1, :].astype(F32)).astype(BF16)
            return carry
        lax.fori_loop(0, chips, body, 0, unroll=4)

    tail = ff - (ff_tiles - 1) * head
    with jax.named_scope('zeros'):
        for l in range(layers):
            for i in range(2):
                lo = (ff_tiles - 1) * TILE + i * head + tail // 16 * 16
                hi = (ff_tiles - 1) * TILE + (i + 1) * head
                wgu[l, lo:hi, :] = jnp.zeros((hi - lo, width), BF16)
                lo = i * kdim + (head + ff) // 16 * 16
                wod[l, lo:(i + 1) * kdim, :] = jnp.zeros(((i + 1) * kdim - lo, half), BF16)
    pl.semaphore_signal(bar, inc=1, device_id=partner)
    for k in range(1, chips):
        pl.semaphore_signal(bar, inc=1, device_id=dev(shift(py, k // side), shift(px, k % side), core))
    wait(smalls)
    with jax.named_scope('tables'):
        lane = lax.broadcasted_iota(jnp.int32, (128, head), 1)
        for i in range(len_in.shape[0]):
            pos_rows = jnp.broadcast_to(len_in[i:i + 1, :].astype(F32), (128, 128)).T
            len_ref[i * 128:(i + 1) * 128, :] = pos_rows[:, 0:1].astype(jnp.int32)
            angle = pos_rows[:, 0:head] * freq_ref[...]
            cos_ref[i * 128:(i + 1) * 128, :] = jnp.cos(angle)
            sin = jnp.sin(angle)
            sin_ref[i * 128:(i + 1) * 128, :] = jnp.where(lane < head // 2, -sin, sin)
    with jax.named_scope('wait_x'):
        wait([x_load(0)])
    start(gu_loads(0) + cache_loads(0, 0) + od_own(0))
    with jax.named_scope('norm_00'):
        norm_rows(0)
    def enter():
        with jax.named_scope('barrier'):
            pl.semaphore_wait(bar, chips)
        start(od_partner(0))
        for l in range(1, layers):
            start(qkv_loads(l) + gu_loads(l) + od_own(l) + od_partner(l))

    for b in range(1, BLOCKS):
        start([x_load(b)] + cache_loads(0, b))
    for b in range(BLOCKS):
        start([pltpu.make_async_copy(x_hbm.at[b, py, px, :, my_cols], x_own.at[b], own_sem.at[b])])

    part = rows / 256

    def chain(b):
        for l in range(layers):
            yield from compute(l, b)
            yield from finish(l, b)

    def compute(l, b):
        if b == 0:
            with jax.named_scope(f'wait_qkv_{l}{b}'):
                wait(qkv_loads(l))
        if l == 0 and b > 0:
            with jax.named_scope(f'norm_{l}{b}'):
                wait([x_load(b)])
                norm_rows(b)
            yield 1.4 * part, 0, 0, False
        r0 = b * rows
        with jax.named_scope(f'qkv_{l}{b}'):
            a = a_buf[b].reshape(rows, width)
            qkv = jnp.dot(a, wqkv[l], preferred_element_type=F32).astype(BF16)
            cosv, sinv = cos_ref[r0:r0 + rows, :], sin_ref[r0:r0 + rows, :]

            def rope(v):
                v = v.astype(F32)
                return (v * cosv + pltpu.roll(v, head // 2, 1) * sinv).astype(BF16)

            qr, kr = rope(qkv[:, :head]), rope(qkv[:, head:2 * head])
            q_s[b] = qr
            v_s[b] = qkv[:, 2 * head:]
            self_s[b] = jnp.sum(qr.astype(F32) * kr.astype(F32), axis=-1, keepdims=True) * scale
        yield 1.5 * part, 0, 0, False
        if l == 0 and b == 0:
            enter()
        with jax.named_scope(f'wait_gu_{l}{b}'):
            if b == 0:
                wait(gu_loads(l))
        if l > 0:
            for i in range(2):
                h_send(b, i).wait_send()
        for j in range(ff_tiles):
            with jax.named_scope(f'gu_{l}{b}'):
                gu = lax.dot_general(a_buf[b].reshape(rows, width), wgu[l, j * TILE:(j + 1) * TILE, :], NT, preferred_element_type=F32)
                gate = gu[:, :head].astype(BF16).astype(F32)
                up = gu[:, head:].astype(BF16).astype(F32)
                h_buf[b, core, :, (j + 1) * head:(j + 2) * head] = (gate * jax.nn.sigmoid(gate) * up).astype(BF16)
            if j + 1 == ff_tiles:
                h_send(b, 1).start()
            yield 0.8 * part, 0, 0, False
        with jax.named_scope(f'wait_cache_{l}{b}'):
            wait(cache_loads(l, b))
        grp = 16
        unroll = 4

        def group(g):
            return pl.ds(pl.multiple_of(g * grp, grp), grp), pl.ds(pl.multiple_of(g * grp * seq, grp * seq), grp * seq)

        def score(i, carry):
            for u in range(unroll):
                sl, ks = group(i * unroll + u)
                lg_s[b, sl, :] = lax.dot_general(q_s[b, sl, :], kbuf[b, ks, :], NT, preferred_element_type=F32)
            return carry

        def soften():
            row_id = lax.rem(lax.broadcasted_iota(jnp.int32, (rows, grp * seq), 0), grp)
            dist = lax.broadcasted_iota(jnp.int32, (rows, grp * seq), 1) - row_id * seq
            logits = jnp.where((dist >= 0) & (dist < len_ref[r0:r0 + rows, :]), lg_s[b] * scale, -jnp.inf)
            own = self_s[b]
            peak = jnp.maximum(jnp.max(logits, axis=-1, keepdims=True), own)
            w = jnp.exp(logits - peak)
            own_w = jnp.exp(own - peak)
            inv = 1.0 / (jnp.sum(w, axis=-1, keepdims=True) + own_w)
            pr_s[b] = (w * inv).astype(BF16)
            ow_s[b] = (own_w * inv).astype(BF16).astype(F32)

        def mix(i, carry):
            for u in range(unroll):
                sl, ks = group(i * unroll + u)
                o = jnp.dot(pr_s[b, sl, :], vbuf[b, ks, :], preferred_element_type=F32) + ow_s[b, sl, :] * v_s[b, sl, :].astype(F32)
                h_buf[b, core, sl, 0:head] = o.astype(BF16)
            return carry

        with jax.named_scope(f'score_{l}{b}'):
            lax.fori_loop(0, rows // grp // unroll, score, 0)
        with jax.named_scope(f'soften_{l}{b}'):
            soften()
        with jax.named_scope(f'mix_{l}{b}'):
            lax.fori_loop(0, rows // grp // unroll, mix, 0)
        h_send(b, 0).start()
        if l + 1 < layers:
            start(cache_loads(l + 1, b))
        yield 2.2 * part, 0, 1.5, False
        with jax.named_scope(f'wait_down_{l}{b}'):
            if b == 0:
                wait(od_own(l))
                for cp in od_partner(l):
                    cp.wait_recv()
            for i in range(2):
                h_send(b, i).wait_recv()
        for hf in range(2):
            with jax.named_scope(f'down_{l}{b}'):
                if l > 0:
                    for k in range(1, side):
                        p1_copy(b, hf, k).wait_send()
                for j in range(hf * quarter // TILE, (hf + 1) * quarter // TILE):
                    cols = slice(j * TILE, (j + 1) * TILE)
                    y = jnp.dot(h_buf[b, 0], wod[l, 0:kdim, cols], preferred_element_type=F32) + jnp.dot(h_buf[b, 1], wod[l, kdim:2 * kdim, cols], preferred_element_type=F32)
                    send[b, :, :, :, cols] = y.astype(BF16).reshape(side, side, toks, TILE)
                for k in far_first:
                    p1_copy(b, hf, k).start()
        yield 1.8 * part, 5.6 * part, 2.2, True

    def h_send(b, i):
        ref = h_buf.at[b, core, :, pl.ds(0, head)] if i == 0 else h_buf.at[b, core, :, pl.ds(head, kdim - head)]
        return pltpu.make_async_remote_copy(ref, ref, h_ssem.at[b, i], h_rsem.at[b, i], device_id=partner)

    far_first = sorted(range(1, side), key=lambda k: -min(k, side - k))

    def pos(hf):
        return (px, py) if hf == 0 else (py, px)

    def at(hf, p1, p2):
        return dev(p2, p1, core) if hf == 0 else dev(p1, p2, core)

    def line_of(ref, b, hf, p1, cols):
        return ref.at[b, :, p1, :, cols] if hf == 0 else ref.at[b, p1, :, :, cols]

    def hf_cols(hf):
        return pl.ds(hf * quarter, quarter)

    def p1_copy(b, hf, k):
        p1, p2 = pos(hf)
        to = shift(p1, k)
        return pltpu.make_async_remote_copy(line_of(send, b, hf, to, hf_cols(hf)), r1.at[b, hf, k - 1], p1_ssem.at[b, hf, k - 1], p1_rsem.at[b, hf, k - 1], device_id=at(hf, to, p2))

    def p2_copy(b, hf, k):
        p1, p2 = pos(hf)
        to = shift(p2, k)
        return pltpu.make_async_remote_copy(mid.at[b, hf, to], r2.at[b, hf, k - 1], p2_ssem.at[b, hf, k - 1], p2_rsem.at[b, hf, k - 1], device_id=at(hf, p1, to))

    def st_copy(b):
        return pltpu.make_async_remote_copy(st_send.at[b], st_recv.at[b], st_sem.at[b, 0], st_sem.at[b, 1], device_id=partner)

    def finish(l, b):
        last = l + 1 == layers
        buf = out_ref if last else a_buf
        if l == 0:
            wait_bytes(x_own.at[b], own_sem.at[b])
        chunk = 256
        for hf in range(2):
            p1, p2 = pos(hf)
            with jax.named_scope(f'wait_p1_{l}{b}'):
                for k in range(1, side):
                    p1_copy(b, hf, k).wait_recv()
                    if l > 0:
                        p2_copy(b, hf, k).wait_send()
            with jax.named_scope(f'mid_{l}{b}'):
                for q in range(side):
                    own = send[b, q, p1, :, hf * quarter:(hf + 1) * quarter] if hf == 0 else send[b, p1, q, :, hf * quarter:(hf + 1) * quarter]
                    acc = own.astype(F32)
                    for k in range(side - 1):
                        acc = acc + r1[b, hf, k, q].astype(F32)
                    mid[b, hf, q] = acc
                for k in far_first:
                    p2_copy(b, hf, k).start()
        yield 0.4 * part, 2.8 * part, 2.2, True
        sq = jnp.zeros((toks, 128), F32)
        for hf in range(2):
            p1, p2 = pos(hf)
            with jax.named_scope(f'wait_p2_{l}{b}'):
                for k in range(1, side):
                    p2_copy(b, hf, k).wait_recv()
            with jax.named_scope(f'reduce_{l}{b}'):
                for c0 in range(0, quarter, chunk):
                    cols = slice(c0, c0 + chunk)
                    xc = slice(hf * quarter + c0, hf * quarter + c0 + chunk)
                    acc = mid[b, hf, p2, :, cols]
                    for k in range(side - 1):
                        acc = acc + r2[b, hf, k, :, cols]
                    xn = (x_own[b, :, xc].astype(F32) + acc).astype(BF16)
                    if last:
                        buf[b, py, px, :, pl.ds(pl.multiple_of(core * half + hf * quarter + c0, chunk), chunk)] = xn
                    else:
                        x_own[b, :, xc] = xn
                        xf = xn.astype(F32)
                        for i in range(chunk // 128):
                            v = xf[:, i * 128:(i + 1) * 128]
                            sq = sq + v * v
        if not last:
            if l > 0:
                st_copy(b).wait_send()
            st_send[b] = sq
            st_copy(b).start()
            yield 0.2 * part, 0, 1.4, True
            with jax.named_scope(f'wait_st_{l}{b}'):
                st_copy(b).wait_recv()
            with jax.named_scope(f'scale_{l}{b}'):
                total = jnp.sum(st_send[b] + st_recv[b], axis=-1, keepdims=True)
                inv = lax.rsqrt(total / width + NORM_EPS)
                for c0 in range(0, half, chunk):
                    cc = pl.ds(pl.multiple_of(core * half + c0, chunk), chunk)
                    buf[b, py, px, :, cc] = (x_own[b, :, c0:c0 + chunk].astype(F32) * inv * gain_ref[l + 1:l + 2, cc].astype(F32)).astype(BF16)
        sgn = 1 - 2 * core

        def place(hf, p1, p2=None):
            first = slice(None) if p1 is None else p1
            y, x = (p2, first) if hf == 0 else (first, p2)
            return buf.at[b, y, x, :, part_cols(hf, core)]

        def copy(hf, ref, target, idx):
            return pltpu.make_async_remote_copy(ref, ref, ag_ssem.at[b, hf, idx], ag_rsem.at[b, hf, idx], device_id=target)

        def to_partner(hf, ref, idx):
            return pltpu.make_async_remote_copy(ref, ref, d_ssem.at[b, hf, idx], d_rsem.at[b, hf, idx], device_id=partner)

        for idx, d in ((2, 2), (0, 1), (1, -1)):
            for hf in range(2):
                p1, p2 = pos(hf)
                copy(hf, place(hf, p1, p2), at(hf, shift(p1, d), p2), idx).start()
        yield 0.2, 1.4 * part, 2.6, True
        with jax.named_scope(f'gather1_{l}{b}'):
            for hf in range(2):
                p1, p2 = pos(hf)
                for idx, d in ((0, -1), (1, 1), (2, 2)):
                    wait_bytes(place(hf, shift(p1, d), p2), ag_rsem.at[b, hf, idx])
                for idx, d in ((3, 1), (4, -1)):
                    copy(hf, place(hf, None, p2), at(hf, p1, shift(p2, d)), idx).start()
                to_partner(hf, place(hf, None, p2), 0).start()
        yield 0.1, 2.8 * part, 2.2, True
        with jax.named_scope(f'gather2_{l}{b}'):
            for hf in range(2):
                p1, p2 = pos(hf)
                src = shift(p2, -sgn)
                line = place(hf, None, src)
                wait_bytes(line, ag_rsem.at[b, hf, 3 + core])
                copy(hf, line, at(hf, p1, shift(p2, sgn)), 5).start()
                to_partner(hf, line, 1).start()
        yield 0.1, 1.4 * part, 0, True
        with jax.named_scope(f'gather3_{l}{b}'):
            for hf in range(2):
                p1, p2 = pos(hf)
                line = place(hf, None, shift(p2, sgn))
                wait_bytes(line, ag_rsem.at[b, hf, 4 - core])
                to_partner(hf, line, 2).start()
        yield 0, 0, 2.2, True
        with jax.named_scope(f'gather4_{l}{b}'):
            for hf in range(2):
                p1, p2 = pos(hf)
                line = place(hf, None, shift(p2, 2))
                wait_bytes(line, ag_rsem.at[b, hf, 5])
                to_partner(hf, line, 3).start()
        yield 0, 0, 1.2, True
        with jax.named_scope(f'gather5_{l}{b}'):
            for hf in range(2):
                p1, p2 = pos(hf)
                for idx in range(4):
                    wait_bytes(place(hf, None, p2), d_rsem.at[b, hf, idx])
                for idx in range(3):
                    wait_bytes(place(hf, p1, p2), ag_ssem.at[b, hf, idx])
                for idx in range(3, 6):
                    wait_bytes(place(hf, None, p2), ag_ssem.at[b, hf, idx])
                for idx in range(4):
                    wait_bytes(place(hf, None, p2), d_ssem.at[b, hf, idx])
    chains = {b: chain(b) for b in range(BLOCKS)}
    ready, light = [0.0] * BLOCKS, [False] * BLOCKS
    now = free = 0.0
    turn = [0, 0]
    while chains:
        if turn:
            b = turn.pop()
        else:
            b = min(chains, key=lambda c: (max(ready[c], now), not light[c], c))
        step = next(chains[b], None)
        if step is None:
            del chains[b]
            continue
        spent, link, delay, light[b] = step
        now = max(now, ready[b]) + spent
        if link:
            free = max(free, now) + link * WIRE
            ready[b] = free + delay
        else:
            ready[b] = now + delay
    for l in range(layers):
        for cp in od_partner(l):
            cp.wait_send()
    for b in range(BLOCKS):
        for i in range(2):
            h_send(b, i).wait_send()
            for k in range(1, side):
                p1_copy(b, i, k).wait_send()
                p2_copy(b, i, k).wait_send()
        if layers > 1:
            st_copy(b).wait_send()


def solution(mesh):
    tp_size = mesh.shape['tp']
    side = math.isqrt(tp_size // 2)
    arg_specs = (P('dp', None), P('dp'), P(), P(None, None, 'tp'), P(None, None, 'tp'), P(None, None, 'tp'), P(None, 'tp', None), P(None, None, 'tp'), P(None, None, 'tp'), P(None, 'tp', None), P(None, 'dp', None, 'tp', None), P(None, 'dp', None, 'tp', None))

    def per_device(x_in, lengths, norm_gain, w_q, w_k, w_v, w_o, w_gate, w_up, w_down, k_cache, v_cache):
        tok_rows, width = x_in.shape
        layers, _, head = w_q.shape
        ff = w_gate.shape[2]
        seq = k_cache.shape[2]
        chips = side * side
        rows = tok_rows // BLOCKS
        toks = rows // chips
        half = width // 2
        ff_tiles = -(-ff // head)
        kdim = head * (1 + ff_tiles)

        inv_freq = (1.0 / (ROPE_BASE ** (np.arange(0, head, 2, dtype=np.float64) / head))).astype(np.float32)
        freq = jnp.asarray(np.concatenate([inv_freq, inv_freq])[None, :])

        any_spec = pl.BlockSpec(memory_space=pl.ANY)
        dma = pltpu.SemaphoreType.DMA
        out = pl.pallas_call(
            functools.partial(layers_kernel, side),
            out_shape=pltpu.VMEM((BLOCKS, side, side, toks, width), BF16),
            in_specs=[any_spec] * 13,
            out_specs=pl.BlockSpec(memory_space=pltpu.VMEM),
            scratch_shapes=[
                pltpu.VMEM((tok_rows // 128, 128), jnp.int32),
                pltpu.VMEM((1, head), F32),
                pltpu.VMEM((layers, width), BF16),
                pltpu.VMEM((tok_rows, 1), jnp.int32),
                pltpu.VMEM((tok_rows, head), F32),
                pltpu.VMEM((tok_rows, head), F32),
                pltpu.VMEM((BLOCKS, rows, 16 * seq), F32),
                pltpu.VMEM((BLOCKS, rows, 16 * seq), BF16),
                pltpu.VMEM((BLOCKS, rows, 1), F32),
                pltpu.VMEM((BLOCKS, side, side, toks, width), BF16),
                pltpu.VMEM((layers, width, 3 * head), BF16),
                pltpu.VMEM((layers, ff_tiles * TILE, width), BF16),
                pltpu.VMEM((layers, 2 * kdim, half), BF16),
                pltpu.VMEM((BLOCKS, rows * seq, head), BF16),
                pltpu.VMEM((BLOCKS, rows * seq, head), BF16),
                pltpu.VMEM((BLOCKS, rows, head), BF16),
                pltpu.VMEM((BLOCKS, rows, head), BF16),
                pltpu.VMEM((BLOCKS, rows, 1), F32),
                pltpu.VMEM((BLOCKS, 2, rows, kdim), BF16),
                pltpu.VMEM((BLOCKS, side, side, toks, half), BF16),
                pltpu.VMEM((BLOCKS, 2, side - 1, side, toks, half // 2), BF16),
                pltpu.VMEM((BLOCKS, 2, side, toks, half // 2), F32),
                pltpu.VMEM((BLOCKS, 2, side - 1, toks, half // 2), F32),
                pltpu.VMEM((BLOCKS, toks, half), BF16),
                pltpu.VMEM((BLOCKS, toks, 128), F32),
                pltpu.VMEM((BLOCKS, toks, 128), F32),
                dma((3,)),
                dma((BLOCKS,)),
                dma((layers, 3 + 2 * ff_tiles)),
                dma((layers, 2)),
                dma((layers, 2)),
                dma((layers, 2)),
                dma((BLOCKS, 2)),
                dma((BLOCKS,)),
                dma((BLOCKS, 2)),
                dma((BLOCKS, 2)),
                dma((BLOCKS, 2, side - 1)),
                dma((BLOCKS, 2, side - 1)),
                dma((BLOCKS, 2, side - 1)),
                dma((BLOCKS, 2, side - 1)),
                dma((BLOCKS, 2)),
                dma((BLOCKS, 2, 6)),
                dma((BLOCKS, 2, 6)),
                dma((BLOCKS, 2, 4)),
                dma((BLOCKS, 2, 4)),
            ],
            compiler_params=pltpu.CompilerParams(collective_id=0, has_side_effects=True, vmem_limit_bytes=58 * 2**20),
            name='decoder_layers',
        )(
            x_in.reshape(BLOCKS, side, side, toks, width),
            lengths.reshape(tok_rows // 128, 128),
            freq,
            norm_gain,
            w_q, w_k, w_v, w_o,
            w_gate.swapaxes(1, 2),
            w_up.swapaxes(1, 2),
            w_down,
            k_cache.reshape(layers, tok_rows * seq, head),
            v_cache.reshape(layers, tok_rows * seq, head),
        )
        return out.reshape(tok_rows, width)

    return jax.shard_map(per_device, mesh=mesh, in_specs=arg_specs, out_specs=P('dp', None), check_vma=False)
```

```python
import functools
import math

import jax
import jax.numpy as jnp
import numpy as np
from jax import lax
from jax.experimental import pallas as pl
from jax.experimental.pallas import tpu as pltpu
from jax.sharding import PartitionSpec as P

NORM_EPS = 1e-5
ROPE_BASE = 500000.0
F32 = jnp.float32
BF16 = jnp.bfloat16
NT = (((1,), (1,)), ((), ()))
BLOCKS = 2
SUBS = 2
WIRE = 1.1
TILE = 256


def wait_bytes(ref, sem):
    pltpu.make_async_copy(ref, ref, sem).wait()


def layers_kernel(side, x_hbm, len_hbm, freq_hbm, gain_hbm, wq, wk, wv, wo, wg, wu, wd, kc, vc, out_ref,
                  len_in, freq_ref, gain_ref, len_ref, cos_ref, sin_ref, lg_s, pr_s, ow_s, a_buf, wqkv, wgu, wod, kbuf, vbuf, q_s, v_s, self_s, h_buf, send, r1, mid, r2, x_own, st_send, st_recv,
                  small_sem, x_sem, w_sem, wo_sem, wp_ssem, wp_rsem, c_sem, own_sem, h_ssem, h_rsem, p1_ssem, p1_rsem, p2_ssem, p2_rsem, st_sem, ag_ssem, ag_rsem, d_ssem, d_rsem):
    layers, width = wq.shape[0], wq.shape[1]
    head = wq.shape[2]
    ff = wd.shape[1]
    half = width // 2
    quarter = width // 4
    toks = x_hbm.shape[3]
    chips = side * side
    rows = SUBS * chips * toks
    seq = kc.shape[1] // (BLOCKS * rows)
    ff_tiles = wgu.shape[1] // TILE
    kdim = h_buf.shape[3]
    scale = head ** -0.5

    me = lax.axis_index('tp')
    core = lax.rem(me, 2)
    chip = lax.div(me, 2)
    px = lax.rem(chip, side)
    py = lax.div(chip, side)
    other = 1 - core

    def dev(y, x, c):
        return {'tp': (y * side + x) * 2 + c}

    def shift(p, d):
        return lax.rem(p + d + side, side)

    partner = dev(py, px, other)
    my_cols = pl.ds(pl.multiple_of(core * half, half), half)
    other_cols = pl.ds(pl.multiple_of(other * half, half), half)

    def part_cols(hf, c):
        return pl.ds(pl.multiple_of(c * half + hf * quarter, quarter), quarter)

    def k_rows(c, start, n):
        return pl.ds(pl.multiple_of(c * kdim + start, 8), n)

    def subs(b):
        return pl.ds(b * SUBS, SUBS)

    def x_load(b):
        return pltpu.make_async_copy(x_hbm.at[subs(b)], out_ref.at[subs(b)], x_sem.at[b])

    def qkv_loads(l):
        return [pltpu.make_async_copy(w.at[l], wqkv.at[l, :, pl.ds(i * head, head)], w_sem.at[l, i]) for i, w in enumerate((wq, wk, wv))]

    def gu_loads(l):
        cps = []
        for j in range(ff_tiles):
            n = min(head, ff - j * head)
            for i, w in enumerate((wg, wu)):
                cps.append(pltpu.make_async_copy(w.at[l, pl.ds(j * head, n)], wgu.at[l, pl.ds(j * TILE + i * head, n)], w_sem.at[l, 3 + 2 * j + i]))
        return cps

    def od_own(l):
        return [
            pltpu.make_async_copy(wo.at[l, :, my_cols], wod.at[l, k_rows(core, 0, head)], wo_sem.at[l, 0]),
            pltpu.make_async_copy(wd.at[l, :, my_cols], wod.at[l, k_rows(core, head, ff)], wo_sem.at[l, 1]),
        ]

    def od_partner(l):
        return [
            pltpu.make_async_remote_copy(wo.at[l, :, other_cols], wod.at[l, k_rows(core, 0, head)], wp_ssem.at[l, 0], wp_rsem.at[l, 0], device_id=partner),
            pltpu.make_async_remote_copy(wd.at[l, :, other_cols], wod.at[l, k_rows(core, head, ff)], wp_ssem.at[l, 1], wp_rsem.at[l, 1], device_id=partner),
        ]

    def cache_loads(l, b):
        span = pl.ds(b * rows * seq, rows * seq)
        return [
            pltpu.make_async_copy(kc.at[l, span], kbuf.at[b], c_sem.at[b, 0]),
            pltpu.make_async_copy(vc.at[l, span], vbuf.at[b], c_sem.at[b, 1]),
        ]

    def start(cps):
        for cp in cps:
            cp.start()

    def wait(cps):
        for cp in cps:
            cp.wait()

    smalls = [pltpu.make_async_copy(src, dst, small_sem.at[i]) for i, (src, dst) in enumerate(((gain_hbm, gain_ref), (len_hbm, len_in), (freq_hbm, freq_ref)))]
    start(smalls + [x_load(0)] + qkv_loads(0))
    bar = pltpu.get_barrier_semaphore()

    def norm_rows(b):
        def body(i, carry):
            sb = b * SUBS + lax.div(i, chips // 2)
            pair = lax.rem(i, chips // 2)
            y, x = lax.div(pair, side // 2), pl.ds(lax.rem(pair, side // 2) * 2, 2)
            xv = out_ref[sb, y, x].astype(F32)
            inv = lax.rsqrt(jnp.mean(xv * xv, axis=-1, keepdims=True) + NORM_EPS)
            a_buf[sb, y, x] = (xv * inv * gain_ref[0:1, :].astype(F32)).astype(BF16)
            return carry
        lax.fori_loop(0, SUBS * chips // 2, body, 0, unroll=4)

    tail = ff - (ff_tiles - 1) * head
    with jax.named_scope('zeros'):
        for l in range(layers):
            for i in range(2):
                lo = (ff_tiles - 1) * TILE + i * head + tail // 16 * 16
                hi = (ff_tiles - 1) * TILE + (i + 1) * head
                wgu[l, lo:hi, :] = jnp.zeros((hi - lo, width), BF16)
                lo = i * kdim + (head + ff) // 16 * 16
                wod[l, lo:(i + 1) * kdim, :] = jnp.zeros(((i + 1) * kdim - lo, half), BF16)
    pl.semaphore_signal(bar, inc=1, device_id=partner)
    for k in range(1, chips):
        pl.semaphore_signal(bar, inc=1, device_id=dev(shift(py, k // side), shift(px, k % side), core))
    wait(smalls)
    with jax.named_scope('tables'):
        lane = lax.broadcasted_iota(jnp.int32, (128, head), 1)
        for i in range(len_in.shape[0]):
            pos_rows = jnp.broadcast_to(len_in[i:i + 1, :].astype(F32), (128, 128)).T
            len_ref[i * 128:(i + 1) * 128, :] = pos_rows[:, 0:1].astype(jnp.int32)
            angle = pos_rows[:, 0:head] * freq_ref[...]
            cos_ref[i * 128:(i + 1) * 128, :] = jnp.cos(angle)
            sin = jnp.sin(angle)
            sin_ref[i * 128:(i + 1) * 128, :] = jnp.where(lane < head // 2, -sin, sin)
    with jax.named_scope('wait_x'):
        wait([x_load(0)])
    start(gu_loads(0) + cache_loads(0, 0) + od_own(0))
    with jax.named_scope('norm_00'):
        norm_rows(0)
    def enter():
        with jax.named_scope('barrier'):
            pl.semaphore_wait(bar, chips)
        start(od_partner(0))
        for l in range(1, layers):
            start(qkv_loads(l) + gu_loads(l) + od_own(l) + od_partner(l))

    for b in range(1, BLOCKS):
        start([x_load(b)] + cache_loads(0, b))
    for b in range(BLOCKS * SUBS):
        start([pltpu.make_async_copy(x_hbm.at[b, py, px, :, my_cols], x_own.at[b], own_sem.at[b])])

    part = rows / 256
    share = part / SUBS

    def compute_chain(b):
        for l in range(layers):
            yield from compute(l, b)

    def finish_chain(sb):
        for l in range(layers):
            yield from finish(l, sb)

    def compute(l, b):
        if b == 0:
            with jax.named_scope(f'wait_qkv_{l}{b}'):
                wait(qkv_loads(l))
        if l == 0 and b > 0:
            with jax.named_scope(f'norm_{l}{b}'):
                wait([x_load(b)])
                norm_rows(b)
            yield 1.4 * part, 0, 0, False
        r0 = b * rows
        with jax.named_scope(f'qkv_{l}{b}'):
            a = a_buf[subs(b)].reshape(rows, width)
            qkv = jnp.dot(a, wqkv[l], preferred_element_type=F32).astype(BF16)
            cosv, sinv = cos_ref[r0:r0 + rows, :], sin_ref[r0:r0 + rows, :]

            def rope(v):
                v = v.astype(F32)
                return (v * cosv + pltpu.roll(v, head // 2, 1) * sinv).astype(BF16)

            qr, kr = rope(qkv[:, :head]), rope(qkv[:, head:2 * head])
            q_s[b] = qr
            v_s[b] = qkv[:, 2 * head:]
            self_s[b] = jnp.sum(qr.astype(F32) * kr.astype(F32), axis=-1, keepdims=True) * scale
        yield 1.5 * part, 0, 0, False
        if l == 0 and b == 0:
            enter()
        with jax.named_scope(f'wait_gu_{l}{b}'):
            if b == 0:
                wait(gu_loads(l))
        if l > 0:
            for i in range(2):
                h_send(b, i).wait_send()
        for j in range(ff_tiles):
            with jax.named_scope(f'gu_{l}{b}'):
                gu = lax.dot_general(a_buf[subs(b)].reshape(rows, width), wgu[l, j * TILE:(j + 1) * TILE, :], NT, preferred_element_type=F32)
                gate = gu[:, :head].astype(BF16).astype(F32)
                up = gu[:, head:].astype(BF16).astype(F32)
                h_buf[b, core, :, (j + 1) * head:(j + 2) * head] = (gate * jax.nn.sigmoid(gate) * up).astype(BF16)
            if j + 1 == ff_tiles:
                h_send(b, 1).start()
            yield 0.8 * part, 0, 0, False
        with jax.named_scope(f'wait_cache_{l}{b}'):
            wait(cache_loads(l, b))
        grp = 16
        unroll = 4

        def group(g):
            return pl.ds(pl.multiple_of(g * grp, grp), grp), pl.ds(pl.multiple_of(g * grp * seq, grp * seq), grp * seq)

        def score(i, carry):
            for u in range(unroll):
                sl, ks = group(i * unroll + u)
                lg_s[b, sl, :] = lax.dot_general(q_s[b, sl, :], kbuf[b, ks, :], NT, preferred_element_type=F32)
            return carry

        def soften():
            row_id = lax.rem(lax.broadcasted_iota(jnp.int32, (rows, grp * seq), 0), grp)
            dist = lax.broadcasted_iota(jnp.int32, (rows, grp * seq), 1) - row_id * seq
            logits = jnp.where((dist >= 0) & (dist < len_ref[r0:r0 + rows, :]), lg_s[b] * scale, -jnp.inf)
            own = self_s[b]
            peak = jnp.maximum(jnp.max(logits, axis=-1, keepdims=True), own)
            w = jnp.exp(logits - peak)
            own_w = jnp.exp(own - peak)
            inv = 1.0 / (jnp.sum(w, axis=-1, keepdims=True) + own_w)
            pr_s[b] = (w * inv).astype(BF16)
            ow_s[b] = (own_w * inv).astype(BF16).astype(F32)

        def mix(i, carry):
            for u in range(unroll):
                sl, ks = group(i * unroll + u)
                o = jnp.dot(pr_s[b, sl, :], vbuf[b, ks, :], preferred_element_type=F32) + ow_s[b, sl, :] * v_s[b, sl, :].astype(F32)
                h_buf[b, core, sl, 0:head] = o.astype(BF16)
            return carry

        with jax.named_scope(f'score_{l}{b}'):
            lax.fori_loop(0, rows // grp // unroll, score, 0)
        with jax.named_scope(f'soften_{l}{b}'):
            soften()
        with jax.named_scope(f'mix_{l}{b}'):
            lax.fori_loop(0, rows // grp // unroll, mix, 0)
        h_send(b, 0).start()
        if l + 1 < layers:
            start(cache_loads(l + 1, b))
        yield 2.2 * part, 0, 1.5, False
        with jax.named_scope(f'wait_down_{l}{b}'):
            if b == 0:
                wait(od_own(l))
                for cp in od_partner(l):
                    cp.wait_recv()
            for i in range(2):
                h_send(b, i).wait_recv()
        for hf in range(2):
            with jax.named_scope(f'down_{l}{b}'):
                if l > 0 and hf == 0:
                    for sb in range(b * SUBS, (b + 1) * SUBS):
                        wait_bytes(r1.at[sb], p1_ssem.at[sb])
                for j in range(hf * quarter // TILE, (hf + 1) * quarter // TILE):
                    cols = slice(j * TILE, (j + 1) * TILE)
                    y = jnp.dot(h_buf[b, 0], wod[l, 0:kdim, cols], preferred_element_type=F32) + jnp.dot(h_buf[b, 1], wod[l, kdim:2 * kdim, cols], preferred_element_type=F32)
                    send[subs(b), :, :, :, cols] = y.astype(BF16).reshape(SUBS, side, side, toks, TILE)
                for sb in range(b * SUBS, (b + 1) * SUBS):
                    for k in far_first:
                        p1_copy(sb, hf, k).start()
        needs = [('rows', l, sb) for sb in range(b * SUBS, (b + 1) * SUBS)]
        yield 1.8 * part, 0, 0, False, needs, [(('shares', l, sb), 5.6 * share, 2.2) for sb in range(b * SUBS, (b + 1) * SUBS)]

    def h_send(b, i):
        ref = h_buf.at[b, core, :, pl.ds(0, head)] if i == 0 else h_buf.at[b, core, :, pl.ds(head, kdim - head)]
        return pltpu.make_async_remote_copy(ref, ref, h_ssem.at[b, i], h_rsem.at[b, i], device_id=partner)

    far_first = sorted(range(1, side), key=lambda k: -min(k, side - k))

    def pos(hf):
        return (px, py) if hf == 0 else (py, px)

    def at(hf, p1, p2):
        return dev(p2, p1, core) if hf == 0 else dev(p1, p2, core)

    def line_of(ref, b, hf, p1, cols):
        return ref.at[b, :, p1, :, cols] if hf == 0 else ref.at[b, p1, :, :, cols]

    def hf_cols(hf):
        return pl.ds(hf * quarter, quarter)

    def p1_copy(b, hf, k):
        p1, p2 = pos(hf)
        to = shift(p1, k)
        return pltpu.make_async_remote_copy(line_of(send, b, hf, to, hf_cols(hf)), r1.at[b, hf, k - 1], p1_ssem.at[b], p1_rsem.at[b, hf], device_id=at(hf, to, p2))

    def p2_copy(b, hf, k):
        p1, p2 = pos(hf)
        to = shift(p2, k)
        return pltpu.make_async_remote_copy(mid.at[b, hf, to], r2.at[b, hf, k - 1], p2_ssem.at[b], p2_rsem.at[b, hf], device_id=at(hf, p1, to))

    def st_copy(b):
        return pltpu.make_async_remote_copy(st_send.at[b], st_recv.at[b], st_sem.at[b, 0], st_sem.at[b, 1], device_id=partner)

    def finish(l, b):
        last = l + 1 == layers
        buf = out_ref if last else a_buf
        if l == 0:
            wait_bytes(x_own.at[b], own_sem.at[b])
        chunk = 256
        for hf in range(2):
            p1, p2 = pos(hf)
            with jax.named_scope(f'wait_p1_{l}{b}'):
                wait_bytes(r1.at[b, hf], p1_rsem.at[b, hf])
                if l > 0 and hf == 0:
                    wait_bytes(r2.at[b], p2_ssem.at[b])
            with jax.named_scope(f'mid_{l}{b}'):
                for q in range(side):
                    own = send[b, q, p1, :, hf * quarter:(hf + 1) * quarter] if hf == 0 else send[b, p1, q, :, hf * quarter:(hf + 1) * quarter]
                    acc = own.astype(F32)
                    for k in range(side - 1):
                        acc = acc + r1[b, hf, k, q].astype(F32)
                    mid[b, hf, q] = acc
                for k in far_first:
                    p2_copy(b, hf, k).start()
        yield 0.3 * share, 2.8 * share, 2.2, True
        sq = jnp.zeros((toks, 128), F32)
        for hf in range(2):
            p1, p2 = pos(hf)
            with jax.named_scope(f'wait_p2_{l}{b}'):
                wait_bytes(r2.at[b, hf], p2_rsem.at[b, hf])
            with jax.named_scope(f'reduce_{l}{b}'):
                for c0 in range(0, quarter, chunk):
                    cols = slice(c0, c0 + chunk)
                    xc = slice(hf * quarter + c0, hf * quarter + c0 + chunk)
                    acc = mid[b, hf, p2, :, cols]
                    for k in range(side - 1):
                        acc = acc + r2[b, hf, k, :, cols]
                    xn = (x_own[b, :, xc].astype(F32) + acc).astype(BF16)
                    if last:
                        buf[b, py, px, :, pl.ds(pl.multiple_of(core * half + hf * quarter + c0, chunk), chunk)] = xn
                    else:
                        x_own[b, :, xc] = xn
                        xf = xn.astype(F32)
                        for i in range(chunk // 128):
                            v = xf[:, i * 128:(i + 1) * 128]
                            sq = sq + v * v
        if not last:
            if l > 0:
                st_copy(b).wait_send()
            st_send[b] = sq
            st_copy(b).start()
            yield 0.2 * share, 0, 1.4, True
            with jax.named_scope(f'wait_st_{l}{b}'):
                st_copy(b).wait_recv()
            with jax.named_scope(f'scale_{l}{b}'):
                total = jnp.sum(st_send[b] + st_recv[b], axis=-1, keepdims=True)
                inv = lax.rsqrt(total / width + NORM_EPS)
                for c0 in range(0, half, chunk):
                    cc = pl.ds(pl.multiple_of(core * half + c0, chunk), chunk)
                    buf[b, py, px, :, cc] = (x_own[b, :, c0:c0 + chunk].astype(F32) * inv * gain_ref[l + 1:l + 2, cc].astype(F32)).astype(BF16)
        sgn = 1 - 2 * core

        def place(hf, p1, p2=None):
            first = slice(None) if p1 is None else p1
            y, x = (p2, first) if hf == 0 else (first, p2)
            return buf.at[b, y, x, :, part_cols(hf, core)]

        def copy(hf, ref, target, idx):
            return pltpu.make_async_remote_copy(ref, ref, ag_ssem.at[b], ag_rsem.at[b, hf, max(idx - 2, 0)], device_id=target)

        def to_partner(ref):
            return pltpu.make_async_remote_copy(ref, ref, d_ssem.at[b], d_rsem.at[b], device_id=partner)

        for idx, d in ((2, 2), (0, 1), (1, -1)):
            for hf in range(2):
                p1, p2 = pos(hf)
                copy(hf, place(hf, p1, p2), at(hf, shift(p1, d), p2), idx).start()
        yield 0.2, 1.4 * share, 2.6, True
        with jax.named_scope(f'gather1_{l}{b}'):
            for hf in range(2):
                p1, p2 = pos(hf)
                wait_bytes(place(hf, pl.ds(0, side - 1), p2), ag_rsem.at[b, hf, 0])
                for idx, d in ((3, 1), (4, -1)):
                    copy(hf, place(hf, None, p2), at(hf, p1, shift(p2, d)), idx).start()
                to_partner(place(hf, None, p2)).start()
        yield 0.1, 2.8 * share, 2.2, True
        with jax.named_scope(f'gather2_{l}{b}'):
            for hf in range(2):
                p1, p2 = pos(hf)
                src = shift(p2, -sgn)
                line = place(hf, None, src)
                wait_bytes(line, ag_rsem.at[b, hf, 1 + core])
                copy(hf, line, at(hf, p1, shift(p2, sgn)), 5).start()
                to_partner(line).start()
        yield 0.1, 1.4 * share, 0, True
        with jax.named_scope(f'gather3_{l}{b}'):
            for hf in range(2):
                p1, p2 = pos(hf)
                line = place(hf, None, shift(p2, sgn))
                wait_bytes(line, ag_rsem.at[b, hf, 2 - core])
                to_partner(line).start()
        yield 0, 0, 2.2, True
        with jax.named_scope(f'gather4_{l}{b}'):
            for hf in range(2):
                p1, p2 = pos(hf)
                line = place(hf, None, shift(p2, 2))
                wait_bytes(line, ag_rsem.at[b, hf, 3])
                to_partner(line).start()
        yield 0, 0, 1.2, True
        with jax.named_scope(f'gather5_{l}{b}'):
            wait_bytes(buf.at[b, :, :, :, my_cols], d_rsem.at[b])
            wait_bytes(buf.at[b, :, :, :, my_cols], d_ssem.at[b])
            wait_bytes(buf.at[b, pl.ds(0, side - 1), :, :, my_cols], ag_ssem.at[b])
            wait_bytes(buf.at[b, 0, pl.ds(0, side - 1), :, my_cols], ag_ssem.at[b])
        yield 0, 0, 0, True, [('shares', l + 1, b)], [(('rows', l, b), 0, 0)]

    chains = {b: compute_chain(b) for b in range(BLOCKS)}
    chains.update({BLOCKS + sb: finish_chain(sb) for sb in range(BLOCKS * SUBS)})
    count = len(chains)
    ready, light = [0.0] * count, [c >= BLOCKS for c in range(count)]
    needs = [[] if c < BLOCKS else [('shares', 0, c - BLOCKS)] for c in range(count)]
    known = {}
    now = free = 0.0
    turn = [0, 0]
    while chains:
        able = [c for c in chains if all(n in known for n in needs[c])]
        begin = {c: max([ready[c], now] + [known[n] for n in needs[c]]) for c in able}
        c = turn.pop() if turn else min(able, key=lambda c: (begin[c] - (0.7 if c == 0 else 0), not light[c], c))
        step = next(chains[c], None)
        if step is None:
            del chains[c]
            continue
        spent, link, delay, light[c] = step[:4]
        needs[c], makes = (step[4], step[5]) if len(step) > 4 else ([], [])
        now = begin[c] + spent
        for key, wire, late in [(None, link, delay)] + makes:
            if wire:
                free = max(free, now) + wire * WIRE
            at_time = (free if wire else now) + late
            if key is None:
                ready[c] = at_time
            else:
                known[key] = at_time
        if needs[c] and needs[c][0][1] >= layers or (c < BLOCKS and needs[c] and needs[c][0][1] == layers - 1):
            needs[c] = []
    for l in range(layers):
        for cp in od_partner(l):
            cp.wait_send()
    for b in range(BLOCKS):
        for i in range(2):
            h_send(b, i).wait_send()
    for sb in range(BLOCKS * SUBS):
        wait_bytes(r1.at[sb], p1_ssem.at[sb])
        wait_bytes(r2.at[sb], p2_ssem.at[sb])
        if layers > 1:
            st_copy(sb).wait_send()


def solution(mesh):
    tp_size = mesh.shape['tp']
    side = math.isqrt(tp_size // 2)
    arg_specs = (P('dp', None), P('dp'), P(), P(None, None, 'tp'), P(None, None, 'tp'), P(None, None, 'tp'), P(None, 'tp', None), P(None, None, 'tp'), P(None, None, 'tp'), P(None, 'tp', None), P(None, 'dp', None, 'tp', None), P(None, 'dp', None, 'tp', None))

    def per_device(x_in, lengths, norm_gain, w_q, w_k, w_v, w_o, w_gate, w_up, w_down, k_cache, v_cache):
        tok_rows, width = x_in.shape
        layers, _, head = w_q.shape
        ff = w_gate.shape[2]
        seq = k_cache.shape[2]
        chips = side * side
        rows = tok_rows // BLOCKS
        parts = BLOCKS * SUBS
        toks = tok_rows // parts // chips
        half = width // 2
        ff_tiles = -(-ff // head)
        kdim = head * (1 + ff_tiles)

        inv_freq = (1.0 / (ROPE_BASE ** (np.arange(0, head, 2, dtype=np.float64) / head))).astype(np.float32)
        freq = jnp.asarray(np.concatenate([inv_freq, inv_freq])[None, :])

        any_spec = pl.BlockSpec(memory_space=pl.ANY)
        dma = pltpu.SemaphoreType.DMA
        out = pl.pallas_call(
            functools.partial(layers_kernel, side),
            out_shape=pltpu.VMEM((parts, side, side, toks, width), BF16),
            in_specs=[any_spec] * 13,
            out_specs=pl.BlockSpec(memory_space=pltpu.VMEM),
            scratch_shapes=[
                pltpu.VMEM((tok_rows // 128, 128), jnp.int32),
                pltpu.VMEM((1, head), F32),
                pltpu.VMEM((layers, width), BF16),
                pltpu.VMEM((tok_rows, 1), jnp.int32),
                pltpu.VMEM((tok_rows, head), F32),
                pltpu.VMEM((tok_rows, head), F32),
                pltpu.VMEM((BLOCKS, rows, 16 * seq), F32),
                pltpu.VMEM((BLOCKS, rows, 16 * seq), BF16),
                pltpu.VMEM((BLOCKS, rows, 1), F32),
                pltpu.VMEM((parts, side, side, toks, width), BF16),
                pltpu.VMEM((layers, width, 3 * head), BF16),
                pltpu.VMEM((layers, ff_tiles * TILE, width), BF16),
                pltpu.VMEM((layers, 2 * kdim, half), BF16),
                pltpu.VMEM((BLOCKS, rows * seq, head), BF16),
                pltpu.VMEM((BLOCKS, rows * seq, head), BF16),
                pltpu.VMEM((BLOCKS, rows, head), BF16),
                pltpu.VMEM((BLOCKS, rows, head), BF16),
                pltpu.VMEM((BLOCKS, rows, 1), F32),
                pltpu.VMEM((BLOCKS, 2, rows, kdim), BF16),
                pltpu.VMEM((parts, side, side, toks, half), BF16),
                pltpu.VMEM((parts, 2, side - 1, side, toks, half // 2), BF16),
                pltpu.VMEM((parts, 2, side, toks, half // 2), F32),
                pltpu.VMEM((parts, 2, side - 1, toks, half // 2), F32),
                pltpu.VMEM((parts, toks, half), BF16),
                pltpu.VMEM((parts, toks, 128), F32),
                pltpu.VMEM((parts, toks, 128), F32),
                dma((3,)),
                dma((BLOCKS,)),
                dma((layers, 3 + 2 * ff_tiles)),
                dma((layers, 2)),
                dma((layers, 2)),
                dma((layers, 2)),
                dma((BLOCKS, 2)),
                dma((parts,)),
                dma((BLOCKS, 2)),
                dma((BLOCKS, 2)),
                dma((parts,)),
                dma((parts, 2)),
                dma((parts,)),
                dma((parts, 2)),
                dma((parts, 2)),
                dma((parts,)),
                dma((parts, 2, 4)),
                dma((parts,)),
                dma((parts,)),
            ],
            compiler_params=pltpu.CompilerParams(collective_id=0, has_side_effects=True, vmem_limit_bytes=58 * 2**20),
            name='decoder_layers',
        )(
            x_in.reshape(parts, side, side, toks, width),
            lengths.reshape(tok_rows // 128, 128),
            freq,
            norm_gain,
            w_q, w_k, w_v, w_o,
            w_gate.swapaxes(1, 2),
            w_up.swapaxes(1, 2),
            w_down,
            k_cache.reshape(layers, tok_rows * seq, head),
            v_cache.reshape(layers, tok_rows * seq, head),
        )
        return out.reshape(tok_rows, width)

    return jax.shard_map(per_device, mesh=mesh, in_specs=arg_specs, out_specs=P('dp', None), check_vma=False)
```
